32 devices in a mesh: group: 2 (over x), seq: 16 (over z, y, core).
Axes of the slice: x: 2, y: 2, z: 4, core: 2. Of those that a mesh axis runs over, the one named last changes fastest.
Arguments:
- tokens: bfloat16 [16384, 4096], P(('group', 'seq')), parts along dimension 0, may hold values from -6 to 6
- norm_gain: bfloat16 [4096], replicated, may hold values from 0.099609375 to 1.8984375
- w_key: bfloat16 [4096, 1024], P('seq'), may hold values from -0.09375 to 0.09375
- w_value: bfloat16 [4096, 1024], P('seq'), may hold values from -0.09375 to 0.09375
- lengths: int32 [4], P('group'), parts along dimension 0, may hold values from 2048 to 4096
- page_table: int32 [1024], P(('group', 'seq')), parts along dimension 0, may hold values from 0 to 639, as said below
Outputs:
- kv_cache: bfloat16 [2, 1280, 16, 1024], P(None, ('group', 'seq')), parts along dimension 1
The draws below stay inside these ranges and needn't reach their ends.
There are 2 independent parts, one for each index of `group`. The reference program is written for one: setup_inputs(seed, part) draws one part's arguments, and reference() takes and returns one part's arrays. A program takes and returns all parts, laid end to end along the dimension named above; an argument that names none is the same for every part. Nothing has to cross between parts.
Inputs may be any that keep to these rules, and one draw needn't show every extreme that they name: The entries are distinct. Page g of the 32 pages of device s goes to slot page_table[g] of decode device page_table[g] // 40, which is s + k modulo 16 for an offset k in -2 .. 2, at a slot of the block of 8 slots from (k + 2) * 8 on; so at most 8 pages go from one device to one decode device, and exactly 8 from every device to some decode device.
All inputs are finite; a program needn't handle non-finite values.
Results may differ from the reference program's by a relative error of at most 0.0049.
Values may be sent and summed in bfloat16 or wider, within the bound.
A program may use at most 64 MiB of HBM per device.

```python
import jax
import jax.numpy as jnp
from jax import lax

D = 4096
HEAD = 128
PAGE = 16
REACH = 2
TOK_DEV = 512
KVD = 1024
TOKENS = 8192
LENGTH = 4096
CAP = 8
SLOTS = 40
PAGES = 512
N_SEQ = 16


def draw_page_table(key, part):
    pages_dev = TOK_DEV // PAGE
    regions = 2 * REACH + 1

    def one_device(device):
        device_key = jax.random.fold_in(jax.random.fold_in(key, 7), device)
        first_key, second_key, third_key = jax.random.split(device_key, 3)
        full_region = jax.random.randint(first_key, (), 0, regions)
        ranks = jax.random.permutation(second_key, SLOTS)
        region_of = jnp.arange(SLOTS, dtype=jnp.int32) // CAP
        score = jnp.where(region_of == full_region, 0, SLOTS) + ranks
        order = jnp.argsort(score, stable=True)
        chosen = jax.random.permutation(third_key, order[:pages_dev])
        offset = chosen // CAP - REACH
        target = (device + offset) % N_SEQ
        return (target * SLOTS + chosen).astype(jnp.int32)
    table = jax.vmap(one_device)(jnp.arange(N_SEQ, dtype=jnp.int32))
    return table.reshape(-1).astype(jnp.int32)


def block_levels(key, shape, shards, low, top_value):
    factor_of = 1.0
    for axis_at, parts in shards:
        heights = jax.random.uniform(jax.random.fold_in(jax.random.fold_in(key, 6), axis_at), (parts,), jnp.float32, low / len(shards), top_value / len(shards))
        factor_of = factor_of * jnp.repeat(jnp.exp(heights), shape[axis_at] // parts).reshape((-1,) + (1,) * (len(shape) - 1 - axis_at))
    return factor_of


def bell_draw(own_key, extent, spread, most, cuts=(), kind=jnp.bfloat16):
    values = jax.random.normal(own_key, extent, jnp.float32) * spread
    if len(cuts) > 0:
        values = block_levels(own_key, extent, cuts, -0.22, 0.18) * values
    return jnp.clip(values, min=-most, max=most).astype(kind)


def setup_inputs(seed: int = 0, part: int = 0) -> dict:
    key_list = jax.random.split(jax.random.key(seed), 7)
    part_splits = jax.random.split(jax.random.fold_in(key_list[6], part), 7)
    return {
        "tokens": bell_draw(part_splits[0], (TOKENS, D), 1.0, 6.0, ((0, 16),)),
        "norm_gain": jnp.clip(1.0 + 0.18 * jax.random.normal(key_list[1], (D,), jnp.float32), 0.099609375, 1.8984375).astype(jnp.bfloat16),
        "w_key": bell_draw(key_list[2], (D, KVD), D ** -0.5, 0.09375, ((0, 16),)),
        "w_value": bell_draw(key_list[3], (D, KVD), D ** -0.5, 0.09375, ((0, 16),)),
        "lengths": jax.random.randint(part_splits[4], (2,), LENGTH // 2, LENGTH + 1).astype(jnp.int32),
        "page_table": draw_page_table(jax.random.fold_in(jax.random.fold_in(key_list[6], part), 71), part),
    }


ROPE_THETA = 500000.0
EPS = 1e-05

def rotate_keys(key_rows, position):
    half = HEAD // 2
    freq = ROPE_THETA ** (-(jnp.arange(half, dtype=jnp.float32) * 2.0 / HEAD))
    angle = position.astype(jnp.float32)[:, None] * freq[None, :]
    cosine = jnp.cos(angle)[:, None, :]
    sine = jnp.sin(angle)[:, None, :]
    shaped = key_rows.reshape(key_rows.shape[0], -1, HEAD)
    first = shaped[:, :, :half]
    second = shaped[:, :, half:]
    turned = jnp.concatenate([first * cosine - second * sine, second * cosine + first * sine], axis=2)
    return turned.reshape(key_rows.shape)

def reference(tokens, norm_gain, w_key, w_value, lengths, page_table):
    wide = tokens.astype(jnp.float32)
    scale = lax.rsqrt(lax.optimization_barrier(jnp.mean(wide * wide, axis=1, keepdims=True)) + EPS)
    normed = (wide * scale * norm_gain.astype(jnp.float32)[None, :]).astype(jnp.bfloat16)
    key_rows = jnp.dot(normed, w_key, preferred_element_type=jnp.float32)
    value_rows = jnp.dot(normed, w_value, preferred_element_type=jnp.float32)
    token_index = jnp.arange(TOKENS, dtype=jnp.int32)
    prompt_id = token_index // LENGTH
    position = token_index % LENGTH
    limit = jnp.where(prompt_id == 0, lengths[0], lengths[1])
    inside = (position < limit)[:, None]
    key_rows = rotate_keys(key_rows, position)
    keys = jnp.where(inside, key_rows, 0.0).astype(jnp.bfloat16)
    values = jnp.where(inside, value_rows, 0.0).astype(jnp.bfloat16)
    pages = jnp.stack([keys, values]).reshape(2, PAGES, PAGE, KVD)
    cache = jnp.zeros((2, N_SEQ * SLOTS, PAGE, KVD), jnp.bfloat16)
    return cache.at[:, page_table.astype(jnp.int32)].set(pages)
```

```python
import functools

import jax
import jax.numpy as jnp
import numpy as np
from jax import lax
from jax.experimental import pallas as pl
from jax.experimental.pallas import tpu as pltpu
from jax.sharding import PartitionSpec as P

HEAD = 128
PAGE = 16
REACH = 2
CAP = 8
SLOTS = 40
REGIONS = 2 * REACH + 1
BLOCK = CAP * PAGE
ROWS = SLOTS * PAGE

ROPE_THETA = 500000.0
EPS = 1e-05

TILE = 256
MESH = pl.DeviceIdType.MESH

PAIRED, SPLIT, TURNED = 0, 1, 2
CHUNKS = ((SPLIT, True), (PAIRED, False), (PAIRED, True), (SPLIT, True), (PAIRED, True), (SPLIT, True), (PAIRED, True), (PAIRED, True))
GROUPS = (1, 1, 1, 1, 1, 1, 1, 1)
RELAYED = (1, 5)

LAYERS = 4
LOOP_CHUNKS = 8

BEGIN, CROSS, ACROSS, ALONG, FACE, SIDE, SETTLE, UP, DOWN, RELAY = range(10)
COMPUTE = (0,0,0,0,0,0,0,0,0,0,0,0,0,0,0,0,0,0,0,0,1,1,1,1,1,1,1,1)
END = (
    ((BEGIN, 0, 0, 0), (BEGIN, 0, 0, 1), (BEGIN, 1, 0, 0), (BEGIN, 1, 0, 1), (BEGIN, 2, 0, 0),),
    (),
    (),
    (),
    (),
    (),
    ((BEGIN, 2, 0, 1),),
    (),
    ((BEGIN, 3, 0, 0), (ALONG, 0, 1, -1), (ALONG, 0, 1, 0), (ALONG, 0, 1, 1),),
    ((CROSS, 0, 0, -1), (CROSS, 0, 0, 0), (CROSS, 0, 0, 1),),
    (),
    (),
    ((CROSS, 1, 0, -1), (CROSS, 1, 0, 0), (CROSS, 1, 0, 1),),
    (),
    ((FACE, 0, 1, -1), (FACE, 0, 1, 0),),
    ((BEGIN, 3, 0, 1), (ALONG, 3, 1, -1), (ALONG, 3, 1, 0),),
    ((BEGIN, 4, 0, 0),),
    ((ALONG, 3, 1, 1), (CROSS, 2, 0, -1), (CROSS, 2, 0, 1),),
    ((CROSS, 2, 0, 0), (ALONG, 1, 1, -1), (ALONG, 1, 1, 0),),
    ((ACROSS, 1, 0, -1), (ACROSS, 1, 0, 0), (ACROSS, 1, 0, 1),),
    ((BEGIN, 4, 0, 1), (ALONG, 2, 1, -1), (ALONG, 2, 1, 0), (FACE, 3, 1, -1), (FACE, 3, 1, 0), (SETTLE, 0, 1, -1),
     (SETTLE, 0, 1, 0), (BEGIN, 5, 0, 0), (ALONG, 0, 2, -1), (ALONG, 0, 2, 0), (ALONG, 0, 2, 1),
     (BEGIN, 5, 0, 1), (CROSS, 3, 0, -1), (CROSS, 3, 0, 1), (FACE, 1, 1, -1), (FACE, 1, 1, 0), (ALONG, 1, 2, -1),
     (ALONG, 1, 2, 0), (CROSS, 3, 0, 0), (BEGIN, 6, 0, 0), (FACE, 0, 2, -1), (FACE, 0, 2, 0), (BEGIN, 7, 0, 0),
     (BEGIN, 6, 0, 1), (ALONG, 2, 2, -1), (ALONG, 2, 2, 0), (SETTLE, 3, 1, -1), (SETTLE, 3, 1, 0),
     (FACE, 2, 1, -1), (FACE, 2, 1, 0), (ALONG, 3, 2, -1), (ALONG, 3, 2, 0), (ALONG, 3, 2, 1), (SETTLE, 0, 2, -1),
     (SETTLE, 0, 2, 0), (BEGIN, 7, 0, 1), (ALONG, 0, 3, -1), (ALONG, 0, 3, 0), (ALONG, 0, 3, 1),
     (FACE, 1, 2, -1), (FACE, 1, 2, 0), (CROSS, 4, 0, -1), (CROSS, 4, 0, 0), (CROSS, 4, 0, 1), (ALONG, 4, 1, -1),
     (ALONG, 4, 1, 0), (FACE, 2, 2, -1), (FACE, 2, 2, 0), (FACE, 0, 3, -1), (FACE, 0, 3, 0), (ALONG, 4, 2, -1),
     (ALONG, 4, 2, 0), (FACE, 3, 2, -1), (FACE, 3, 2, 0), (CROSS, 5, 0, -1), (CROSS, 5, 0, 0), (CROSS, 5, 0, 1),
     (ALONG, 1, 3, -1), (ALONG, 1, 3, 0), (SETTLE, 0, 3, -1), (SETTLE, 0, 3, 0), (FACE, 4, 1, -1),
     (FACE, 4, 1, 0), (SETTLE, 3, 2, -1), (SETTLE, 3, 2, 0), (ALONG, 2, 3, -1), (ALONG, 2, 3, 0),
     ),
    ((FACE, 4, 2, -1), (FACE, 4, 2, 0), (ALONG, 5, 1, -1), (ALONG, 5, 1, 0), (ALONG, 5, 1, 1), (CROSS, 6, 0, -1),
     (CROSS, 6, 0, 0), (CROSS, 6, 0, 1), (ALONG, 5, 2, -1), (ALONG, 5, 2, 0), (ALONG, 5, 2, 1),
     (FACE, 1, 3, -1), (FACE, 1, 3, 0), (ALONG, 3, 3, -1), (ALONG, 3, 3, 0), (ALONG, 3, 3, 1), (CROSS, 7, 0, -1),
     (CROSS, 7, 0, 1), (DOWN, 0, 0, 0), (UP, 0, 0, 0), (CROSS, 7, 0, 0),),
    ((FACE, 2, 3, -1), (FACE, 2, 3, 0), (ALONG, 6, 1, -1), (ALONG, 6, 1, 0), (FACE, 3, 3, -1), (FACE, 3, 3, 0),
     (FACE, 5, 1, -1), (FACE, 5, 1, 0), (DOWN, 1, 0, 0), (UP, 1, 0, 0),),
    ((ALONG, 6, 2, -1), (ALONG, 6, 2, 0), (FACE, 5, 2, -1), (FACE, 5, 2, 0), (SETTLE, 3, 3, -1),
     (SETTLE, 3, 3, 0), (DOWN, 2, 0, 0), (UP, 2, 0, 0), (ALONG, 4, 3, -1), (ALONG, 4, 3, 0), (SETTLE, 5, 1, -1),
     (SETTLE, 5, 1, 0), (FACE, 6, 1, -1), (FACE, 6, 1, 0), (ALONG, 5, 3, -1), (ALONG, 5, 3, 0),
     (ALONG, 5, 3, 1),),
    ((DOWN, 3, 0, 0), (UP, 3, 0, 0), (SETTLE, 5, 2, -1), (SETTLE, 5, 2, 0), (FACE, 6, 2, -1), (FACE, 6, 2, 0),
     (ALONG, 7, 1, -1), (ALONG, 7, 1, 0), (FACE, 4, 3, -1), (FACE, 4, 3, 0), (ALONG, 7, 2, -1),
     (ALONG, 7, 2, 0), (FACE, 5, 3, -1), (FACE, 5, 3, 0),),
    ((DOWN, 4, 0, 0), (UP, 4, 0, 0), (FACE, 7, 1, -1), (FACE, 7, 1, 0), (ALONG, 6, 3, -1), (ALONG, 6, 3, 0),
     (SETTLE, 5, 3, -1), (SETTLE, 5, 3, 0), (FACE, 7, 2, -1), (FACE, 7, 2, 0),),
    ((DOWN, 5, 0, 0), (UP, 5, 0, 0), (FACE, 6, 3, -1), (FACE, 6, 3, 0), (ALONG, 7, 3, -1), (ALONG, 7, 3, 0),
     ),
    ((DOWN, 6, 0, 0), (UP, 6, 0, 0), (FACE, 7, 3, -1), (FACE, 7, 3, 0),),
    ((DOWN, 7, 0, 0), (UP, 7, 0, 0),),
)
INNER = (
    ((BEGIN, 0, 0, 0), (BEGIN, 0, 0, 1), (BEGIN, 0, 0, 2), (BEGIN, 1, 0, 0), (BEGIN, 1, 0, 1), (BEGIN, 1, 0, 2),
     (BEGIN, 2, 0, 0), (BEGIN, 2, 0, 1), (BEGIN, 2, 0, 2),),
    (),
    (),
    ((BEGIN, 3, 0, 0),),
    ((BEGIN, 3, 0, 1),),
    ((BEGIN, 4, 0, 0),),
    (),
    ((CROSS, 0, 0, -1), (CROSS, 0, 0, 0), (CROSS, 0, 0, 1), (BEGIN, 5, 0, 0), (BEGIN, 3, 0, 2),
     ),
    (),
    ((BEGIN, 6, 0, 0), (CROSS, 1, 0, -1), (CROSS, 1, 0, 0), (CROSS, 1, 0, 1), (CROSS, 1, 0, 2),
     ),
    ((BEGIN, 7, 0, 0),),
    ((CROSS, 2, 0, -1), (CROSS, 2, 0, 0), (CROSS, 2, 0, 1), (CROSS, 2, 0, 2),),
    ((BEGIN, 4, 0, 2),),
    ((ACROSS, 0, 0, -1), (ACROSS, 0, 0, 0), (CROSS, 3, 0, -1), (CROSS, 3, 0, 0), (CROSS, 3, 0, 1),
     ),
    ((ALONG, 0, 2, -1), (ALONG, 0, 2, 0), (ALONG, 0, 2, 1),),
    ((ACROSS, 1, 0, -1), (ACROSS, 1, 0, 0), (BEGIN, 4, 0, 1),),
    ((CROSS, 4, 0, -1),),
    ((ALONG, 1, 2, -1), (ALONG, 1, 2, 0), (ALONG, 1, 2, 1),),
    ((ACROSS, 2, 0, -1), (ACROSS, 2, 0, 0), (CROSS, 5, 0, -1),),
    ((CROSS, 4, 0, 0), (ALONG, 0, 0, -1), (ALONG, 0, 0, 0), (ALONG, 0, 0, 1), (ALONG, 2, 2, -1),
     (ALONG, 2, 2, 0), (ALONG, 2, 2, 1),),
    ((BEGIN, 5, 0, 2), (ACROSS, 3, 0, -1), (ACROSS, 3, 0, 0), (CROSS, 6, 0, -1), (CROSS, 7, 0, -1),
     (BEGIN, 6, 0, 2), (ALONG, 3, 2, -1), (ALONG, 3, 2, 0), (FACE, 0, 2, -1), (FACE, 0, 2, 0), (CROSS, 4, 0, 1),
     (BEGIN, 5, 0, 1), (ALONG, 3, 2, 1), (BEGIN, 7, 0, 2), (ALONG, 1, 0, -1), (ALONG, 1, 0, 0),
     (ALONG, 1, 0, 1), (ALONG, 0, 3, -1), (ALONG, 0, 3, 0), (ALONG, 0, 3, 1), (FACE, 1, 2, -1),
     (FACE, 1, 2, 0), (BEGIN, 6, 0, 1), (ALONG, 2, 0, -1), (ALONG, 2, 0, 0), (ALONG, 2, 0, 1), (CROSS, 5, 0, 0),
     (ALONG, 4, 2, -1), (ALONG, 4, 2, 0), (FACE, 2, 2, -1), (FACE, 2, 2, 0), (CROSS, 4, 0, 2), (ALONG, 1, 3, -1),
     (ALONG, 1, 3, 0), (ALONG, 1, 3, 1), (FACE, 0, 3, -1), (FACE, 0, 3, 0), (BEGIN, 7, 0, 1),),
    ((CROSS, 6, 0, 0), (ALONG, 4, 2, 1), (ALONG, 3, 0, -1), (ALONG, 3, 0, 0), (ALONG, 3, 0, 1),
     (ALONG, 2, 3, -1), (ALONG, 2, 3, 0), (ALONG, 2, 3, 1), (FACE, 3, 2, -1), (FACE, 3, 2, 0), (ALONG, 5, 2, -1),
     (ALONG, 5, 2, 0), (FACE, 1, 3, -1), (FACE, 1, 3, 0), (ACROSS, 4, 0, -1), (ACROSS, 4, 0, 0),
     ),
    ((UP, 1, 0, 0), (DOWN, 1, 0, 0), (CROSS, 6, 0, 1), (CROSS, 7, 0, 0), (CROSS, 5, 0, 1), (UP, 0, 0, 0),
     (DOWN, 0, 0, 0), (ALONG, 4, 0, -1), (ALONG, 4, 0, 0), (ALONG, 4, 0, 1), (ALONG, 3, 3, -1),
     (ALONG, 3, 3, 0), (ALONG, 3, 3, 1), (FACE, 2, 3, -1), (FACE, 2, 3, 0), (ALONG, 5, 2, 1), (ALONG, 6, 2, -1),
     (ALONG, 6, 2, 0),),
    ((FACE, 4, 2, -1), (FACE, 4, 2, 0), (ALONG, 5, 0, -1), (ALONG, 5, 0, 0), (ALONG, 5, 0, 1), (ALONG, 4, 3, -1),
     (ALONG, 4, 3, 0), (ALONG, 4, 3, 1), (FACE, 3, 3, -1), (FACE, 3, 3, 0), (ALONG, 7, 2, -1), (UP, 2, 0, 0),
     (DOWN, 2, 0, 0), (ACROSS, 5, 0, -1), (ACROSS, 5, 0, 0), (CROSS, 7, 0, 1),),
    ((CROSS, 6, 0, 2), (ALONG, 7, 2, 0), (ALONG, 6, 0, -1), (ALONG, 6, 0, 0), (ALONG, 6, 0, 1),
     (ALONG, 5, 3, -1), (ALONG, 5, 3, 0), (ALONG, 5, 3, 1), (ALONG, 6, 2, 1), (FACE, 5, 2, -1),
     (FACE, 5, 2, 0), (UP, 3, 0, 0), (DOWN, 3, 0, 0), (FACE, 4, 3, -1), (FACE, 4, 3, 0),),
    ((CROSS, 7, 0, 2), (ALONG, 6, 3, -1), (ALONG, 6, 3, 0), (ALONG, 6, 3, 1), (RELAY, 1, 0, 0),
     (UP, 4, 0, 0), (DOWN, 4, 0, 0), (ALONG, 7, 0, -1), (ALONG, 7, 0, 0), (ALONG, 7, 0, 1), (FACE, 5, 3, -1),
     (FACE, 5, 3, 0), (ACROSS, 6, 0, -1), (ACROSS, 6, 0, 0), (ALONG, 7, 2, 1),),
    ((DOWN, 5, 0, 0), (UP, 5, 0, 0), (FACE, 6, 2, -1), (FACE, 6, 2, 0), (FACE, 6, 3, -1), (FACE, 6, 3, 0),
     (ALONG, 7, 3, -1), (ALONG, 7, 3, 0), (ALONG, 7, 3, 1), (ACROSS, 7, 0, -1), (ACROSS, 7, 0, 0),
     ),
    ((DOWN, 6, 0, 0), (UP, 6, 0, 0), (FACE, 7, 2, -1), (FACE, 7, 2, 0), (FACE, 7, 3, -1), (FACE, 7, 3, 0),
     ),
    ((DOWN, 7, 0, 0), (UP, 7, 0, 0), (RELAY, 5, 0, 0),),
)


class Work:
    def __init__(self, n, refs, me):
        (self.gain, self.lengths, self.pages, self.freq, self.wide_gain, self.xbuf, self.onehot,
         self.cosine, self.sine) = refs
        self.n, self.me = n, me
        self.tok_rows, self.features = self.xbuf.shape
        self.length_each = self.tok_rows * n // 2
        self.first = lax.rem(me * self.tok_rows, self.length_each)

    def spread_gain(self):
        each = self.gain[...].astype(jnp.float32)
        rows = [each[i : i + 1, :] for i in range(self.features // HEAD)]
        self.wide_gain[...] = jnp.concatenate(rows, axis=1)

    def normalise(self, at, rows_here):
        xbuf = self.xbuf

        def body(i, carry):
            rows = pl.ds(pl.multiple_of(at + i * 32, 32), 32)
            wide = xbuf[rows, :].astype(jnp.float32)
            scale = lax.rsqrt(jnp.mean(wide * wide, axis=1, keepdims=True) + EPS)
            xbuf[rows, :] = (wide * scale * self.wide_gain[...]).astype(jnp.bfloat16)
            return carry

        lax.fori_loop(0, rows_here // 32, body, 0)

    def mark_rows(self):
        tok_rows = self.tok_rows
        second_prompt = (self.me * tok_rows) // self.length_each
        limit = self.lengths[0] + second_prompt * (self.lengths[1] - self.lengths[0])
        page_count = tok_rows // PAGE
        token = lax.broadcasted_iota(jnp.int32, (page_count, tok_rows), 1)
        page = lax.broadcasted_iota(jnp.int32, (page_count, tok_rows), 0)
        used = jnp.where((token // PAGE == page) & (self.first + token < limit), 1.0, 0.0)
        used = used.astype(jnp.bfloat16)
        slot = lax.rem(self.pages[...], SLOTS)

        def hot(i, carry):
            at = i * BLOCK
            row = lax.broadcasted_iota(jnp.int32, (BLOCK, page_count), 0) + at
            held = jnp.where(row // PAGE == slot, 1.0, 0.0).astype(jnp.bfloat16)
            spread = jnp.dot(held, used, preferred_element_type=jnp.float32)
            row = lax.broadcasted_iota(jnp.int32, (BLOCK, tok_rows), 0)
            column = lax.broadcasted_iota(jnp.int32, (BLOCK, tok_rows), 1)
            same = lax.rem(row, PAGE) == lax.rem(column, PAGE)
            self.onehot[pl.ds(pl.multiple_of(at, BLOCK), BLOCK), :] = jnp.where(
                same, spread, 0.0
            ).astype(jnp.bfloat16)
            return carry

        lax.fori_loop(0, REGIONS, hot, 0)

    def angles(self, at, rows_here):
        def turn(i, carry):
            row_at = pl.multiple_of(at + i * 64, 64)
            row = lax.broadcasted_iota(jnp.int32, (64, HEAD), 0) + (self.first + row_at)
            lane = lax.broadcasted_iota(jnp.int32, (64, HEAD), 1)
            angle = row.astype(jnp.float32) * self.freq[...]
            self.cosine[pl.ds(row_at, 64), :] = jnp.cos(angle)
            sined = jnp.sin(angle)
            self.sine[pl.ds(row_at, 64), :] = jnp.where(lane < HEAD // 2, -sined, sined)
            return carry

        lax.fori_loop(0, rows_here // 64, turn, 0)

    def project(self, weights, is_key, put):
        raw = jnp.dot(self.xbuf[...], weights, preferred_element_type=jnp.float32)
        if is_key:
            heads = []
            for head in range(weights.shape[1] // HEAD):
                one = raw[:, head * HEAD : (head + 1) * HEAD]
                heads.append(one * self.cosine[...] + pltpu.roll(one, HEAD // 2, 1) * self.sine[...])
            raw = jnp.concatenate(heads, axis=1)
        placed = jnp.dot(self.onehot[...], raw.astype(jnp.bfloat16), preferred_element_type=jnp.float32)
        put(placed.astype(jnp.bfloat16))


def copy_to(ref, send_sem, recv_sem, group_at, seq_at, dst=None):
    pltpu.make_async_remote_copy(
        src_ref=ref,
        dst_ref=ref if dst is None else dst,
        send_sem=send_sem,
        recv_sem=recv_sem,
        device_id={"group": group_at, "seq": seq_at},
        device_id_type=MESH,
    ).start()


def wait(ref, sem):
    pltpu.make_async_copy(ref, ref, sem).wait()


def line_kernel(
    n, tokens, gain, w_key, w_value, lengths, pages, freq, out,
    wide_gain, wbuf, xbuf, pbuf, rbuf, onehot, cosine, sine,
    load_sem, tok_sem, ys, yr, fr, fq, zi, zo, zr, xs, xo, xr, xq, cs, cr, hs, hr, rs, rr,
):
    chunks, depth = wbuf.shape[0], wbuf.shape[1]
    half, width = wbuf.shape[5], wbuf.shape[6]
    per_kind = chunks // 2
    group = lax.axis_index("group")
    me = lax.axis_index("seq")
    core, y, z = lax.rem(me, 2), lax.rem(me // 2, 2), me // 4
    other_core, other_y, other_group = 1 - core, 1 - y, 1 - group
    high = z // (depth // 2)
    is_end = (z == 0) | (z == depth - 1)

    def at(p):
        return p + high * (depth - 1 - 2 * p)

    def seq_of(z_at, y_at, core_at):
        return (z_at * 2 + y_at) * 2 + core_at

    to_y = seq_of(z, other_y, core)
    to_core = seq_of(z, y, other_core)

    def piece(j, zz, yy, part):
        return wbuf.at[j, zz, yy, core, part]

    def line(j, zz, yy):
        return wbuf.at[j, zz, yy, core]

    def pair(j, zz, part):
        return wbuf.at[j, zz, :, core, part]

    def layer(j, zz):
        return wbuf.at[j, zz, :, core]

    def load(j):
        w_ref = w_key if j < per_kind else w_value
        columns = pl.ds((j % per_kind) * width, width)
        return [
            pltpu.make_async_copy(
                w_ref.at[pl.ds(part * half, half), columns], piece(j, z, y, part), load_sem.at[j, part]
            )
            for part in range(2)
        ]

    for j in range(chunks):
        for copy in load(j):
            copy.start()
    token_copy = pltpu.make_async_copy(tokens, xbuf, tok_sem)
    token_copy.start()

    barrier = pltpu.get_barrier_semaphore()

    def greet(group_at, seq_at):
        pl.semaphore_signal(
            barrier, inc=1, device_id={"group": group_at, "seq": seq_at}, device_id_type=MESH
        )

    greet(other_group, me)
    for step in range(1, n):
        greet(group, lax.rem(me + step, n))
    pl.semaphore_wait(barrier, n)

    def over_y(ref, j, sem):
        copy_to(ref, ys.at[j], sem, group, to_y)

    def over_x(ref, j, sem):
        copy_to(ref, xs.at[j], sem, other_group, me)

    def inward(ref, j, zz, p):
        copy_to(ref, zi.at[j], zr.at[j, zz], group, seq_of(at(p), y, core))

    def outward(ref, j, zz):
        copy_to(ref, zo.at[j], zr.at[j, zz], group, seq_of(at(0), y, core))

    def to_partner(j, zz):
        copy_to(layer(j, zz), cs.at[j], cr.at[j], group, to_core)

    def loaded(j):
        for copy in load(j):
            copy.wait()

    def end_waits(j, what, k):
        form, both = CHUNKS[j]
        zz = at(k)
        if what == CROSS:
            return [(line(j, z, other_y) if both else piece(j, z, other_y, group), yr.at[j])]
        if what == ACROSS:
            return [(piece(j, z, other_y, other_group), xo.at[j])]
        if what == ALONG:
            return [(pair(j, zz, group) if form == PAIRED else piece(j, zz, y, group), zr.at[j, zz])]
        from_x = (piece(j, zz, y, other_group), xr.at[j, zz])
        from_y = (piece(j, zz, other_y, group), fr.at[j, zz])
        if what == FACE:
            return [(pair(j, zz, other_group), xr.at[j, zz])] if form == PAIRED else [from_x]
        if what == SIDE:
            return [from_y]
        if form == SPLIT:
            return [from_y, (piece(j, zz, other_y, other_group), fq.at[j, zz])]
        return [from_x, (piece(j, zz, other_y, other_group), xq.at[j, zz])]

    def end_sends(j, what, k):
        form, both = CHUNKS[j]
        zz = at(k)
        partner = functools.partial(to_partner, j, zz)
        if what == BEGIN:
            mine = line(j, z, y) if both else piece(j, z, y, group)
            return [lambda: over_y(mine, j, yr.at[j]), lambda: inward(line(j, z, y), j, z, 1)]
        if what == CROSS:
            if both:
                return [lambda: inward(line(j, z, other_y), j, z, 1), lambda: to_partner(j, z)]
            return [
                lambda: inward(piece(j, z, other_y, group), j, z, 1),
                lambda: over_x(piece(j, z, other_y, group), j, xo.at[j]),
            ]
        if what == ACROSS:
            return [lambda: inward(piece(j, z, other_y, other_group), j, z, 1), lambda: to_partner(j, z)]
        if what == ALONG:
            one = piece(j, zz, y, group)
            by_x = lambda: over_x(one, j, xr.at[j, zz])
            by_y = lambda: over_y(one, j, fr.at[j, zz])
            if form == PAIRED:
                return [lambda: over_x(pair(j, zz, group), j, xr.at[j, zz])]
            return [by_x, by_y] if form == SPLIT else [by_y, by_x]
        if what == FACE and form == SPLIT:
            return [lambda: over_y(piece(j, zz, y, other_group), j, fq.at[j, zz])]
        if what == SIDE:
            return [lambda: over_x(piece(j, zz, other_y, group), j, xq.at[j, zz])]
        return [partner]

    def inner_waits(j, what, p):
        zz = at(p)
        if what == CROSS:
            return [(piece(j, z, other_y, group), yr.at[j])]
        if what == ACROSS:
            return [(piece(j, z, other_y, other_group), xo.at[j])]
        if what == ALONG:
            return [(layer(j, zz) if p == 0 else pair(j, zz, group), zr.at[j, zz])]
        return [(pair(j, zz, other_group), xr.at[j, zz])]

    def inner_sends(j, what, p):
        form, _ = CHUNKS[j]
        zz = at(p)
        if what == BEGIN:
            mine = piece(j, z, y, group)
            return [
                lambda: over_y(mine, j, yr.at[j]),
                lambda: outward(mine, j, z),
                lambda: inward(mine, j, z, 2),
            ]
        if what == CROSS:
            crossed = piece(j, z, other_y, group)
            out_too = [lambda: outward(crossed, j, z)] if form == PAIRED else []
            return [lambda: inward(crossed, j, z, 2)] + out_too + [lambda: over_x(crossed, j, xo.at[j])]
        if what == ACROSS:
            return [lambda: to_partner(j, z)]
        if what == ALONG and p == 0:
            return [lambda: inward(pair(j, zz, group), j, zz, 2), lambda: to_partner(j, zz)]
        if what == ALONG:
            kept = pair(j, zz, group) if form == PAIRED else piece(j, zz, y, group)
            return [lambda: outward(kept, j, zz), lambda: over_x(pair(j, zz, group), j, xr.at[j, zz])]
        return [lambda: to_partner(j, zz)]

    first_chunk = [sum(GROUPS[:g]) for g in range(len(GROUPS))]

    def spot(g, region):
        j, wide = first_chunk[g], GROUPS[g] * width
        rows = pl.ds(region * BLOCK, BLOCK)
        return (
            pbuf.at[g, rows, pl.ds(0, wide)],
            out.at[j // per_kind, rows, pl.ds((j % per_kind) * width, wide)],
        )

    def page_to(g, region):
        src, dst = spot(g, region)
        there = lax.rem(me + region - REACH + n, n)
        z_there, y_there = there // 4, lax.rem(there // 2, 2)

        def direct():
            copy_to(src, hs.at[g, region], hr.at[g, region], group, there, dst)

        if g not in RELAYED:
            direct()
            return
        slot = 0 if abs(region - REACH) == 2 else 1
        around = ((z_there == 0) | (z_there == depth - 1)) & (z_there != z)
        z_by = 1 + (z_there // (depth - 1)) * (depth - 3)
        by = seq_of(z_by, y_there, lax.rem(there, 2))

        @pl.when(around)
        def _():
            held = rbuf.at[RELAYED.index(g), slot, :, pl.ds(0, GROUPS[g] * width)]
            copy_to(src, hs.at[g, region], rr.at[g, slot], group, by, held)

        @pl.when(jnp.logical_not(around))
        def _():
            direct()

    def pages_on_chip(g):
        src, dst = spot(g, REACH)
        pltpu.make_async_copy(src, dst, hr.at[g, REACH]).start()
        for region, on in ((3, core == 0), (1, core == 1)):
            @pl.when(on)
            def _():
                src, dst = spot(g, region)
                copy_to(src, hs.at[g, region], hr.at[g, region], group, to_core, dst)

    def pages_off_chip(g, way):
        page_to(g, 4 if way == UP else 0)

        @pl.when(core == (1 if way == UP else 0))
        def _():
            page_to(g, 3 if way == UP else 1)

    def pass_pages(g):
        def one(slot, region):
            held = rbuf.at[RELAYED.index(g), slot, :, pl.ds(0, GROUPS[g] * width)]
            wait(held, rr.at[g, slot])
            _, dst = spot(g, region)
            copy_to(held, rs.at[g, slot], hr.at[g, region], group, seq_of(at(0), y, core), dst)

        for side, regions in ((0, (4, 3)), (1, (0, 1))):
            @pl.when(y == side)
            def _():
                one(0, regions[0])

                @pl.when(core == side)
                def _():
                    one(1, regions[1])

    def run(steps, waits, sends, seen):
        for what, j, k, which in steps:
            if what in (UP, DOWN):
                pages_off_chip(j, what)
            elif what == RELAY:
                pass_pages(j)
            elif what == BEGIN:
                if j not in seen:
                    seen.add(j)
                    loaded(j)
                sends(j, what, k)[which]()
            elif which < 0:
                for ref, sem in waits(j, what, k):
                    wait(ref, sem)
            else:
                sends(j, what, k)[which]()

    work = Work(n, (gain, lengths, pages, freq, wide_gain, xbuf, onehot, cosine, sine), me)
    tok_rows = work.tok_rows

    def project(g):
        at_chunk, wide = first_chunk[g], GROUPS[g] * width
        blocks = []
        for j in range(at_chunk, at_chunk + GROUPS[g]):
            wait(wbuf.at[j, :, :, other_core], cr.at[j])
            blocks.append(wbuf[j].reshape(work.features, width))
        weights = blocks[0] if len(blocks) == 1 else jnp.concatenate(blocks, axis=1)

        def put(placed):
            pbuf[g, :, 0:wide] = placed

        work.project(weights, at_chunk < per_kind, put)
        pages_on_chip(g)

    sixteenth = tok_rows // 16
    jobs = [lambda: (work.spread_gain(), token_copy.wait())]
    jobs += [functools.partial(work.normalise, i * sixteenth, sixteenth) for i in range(16)]
    jobs += [work.mark_rows]
    jobs += [functools.partial(work.angles, i * (tok_rows // 2), tok_rows // 2) for i in range(2)]
    jobs, projects = iter(jobs), iter(range(len(GROUPS)))
    seen_end, seen_inner = set(), set()
    for stretch in range(len(COMPUTE) + 1):
        if stretch:
            if COMPUTE[stretch - 1]:
                project(next(projects))
            else:
                next(jobs)()
        if END[stretch]:

            @pl.when(is_end)
            def _():
                run(END[stretch], end_waits, end_sends, seen_end)

        if INNER[stretch]:

            @pl.when(jnp.logical_not(is_end))
            def _():
                run(INNER[stretch], inner_waits, inner_sends, seen_inner)

    def count(pieces, sem):
        wait(xbuf.at[pl.ds(0, half), pl.ds(0, pieces * width)], sem)

    for j in range(chunks):
        form, both = CHUNKS[j]
        wait(wbuf.at[j, :, :, core], cs.at[j])

        @pl.when(is_end)
        def _():
            far = depth - 1
            count((2 if both else 1) + far * {PAIRED: 0, SPLIT: 2, TURNED: 1}[form], ys.at[j])
            count(far * {PAIRED: 2, SPLIT: 1, TURNED: 2}[form] + (0 if both else 1), xs.at[j])
            count(4, zi.at[j])

        @pl.when(jnp.logical_not(is_end))
        def _():
            count(1, ys.at[j])
            count(2 * depth - 3, xs.at[j])
            count(4, zi.at[j])
            count((depth - 1) * (2 if form == PAIRED else 1), zo.at[j])

    for g in range(len(GROUPS)):
        for region in range(REGIONS):
            src, dst = spot(g, region)
            wait(dst, hr.at[g, region])
            if region != REACH:
                wait(src, hs.at[g, region])
        if g in RELAYED:
            held = rbuf.at[RELAYED.index(g), 0, :, pl.ds(0, GROUPS[g] * width)]

            @pl.when(jnp.logical_not(is_end))
            def _():
                wait(held, rs.at[g, 0])

                @pl.when(core == y)
                def _():
                    wait(held, rs.at[g, 1])


def loop_kernel(
    n, tokens, gain, w_key, w_value, lengths, pages, freq, out,
    wide_gain, wbuf, xbuf, pbuf, onehot, cosine, sine,
    load_sem, tok_sem, ys, yr, zs, zr, xs, xr, cs, cr, hs, hr,
):
    chunks, depth = wbuf.shape[0], wbuf.shape[1]
    half, width = wbuf.shape[5], wbuf.shape[6]
    per_kind = chunks // 2
    group = lax.axis_index("group")
    me = lax.axis_index("seq")
    core, y, z = lax.rem(me, 2), lax.rem(me // 2, 2), me // 4
    other_core, other_y, other_group = 1 - core, 1 - y, 1 - group

    def seq_of(z_at, y_at, core_at):
        return (z_at * 2 + y_at) * 2 + core_at

    def piece(j, z_at, y_at, part):
        return wbuf.at[j, z_at, y_at, core, part]

    loads = []
    for j in range(chunks):
        w_ref = w_key if j < per_kind else w_value
        columns = pl.ds((j % per_kind) * width, width)
        for part in range(2):
            copy = pltpu.make_async_copy(
                w_ref.at[pl.ds(part * half, half), columns], piece(j, z, y, part), load_sem.at[j, part]
            )
            copy.start()
            loads.append(copy)
    token_copy = pltpu.make_async_copy(tokens, xbuf, tok_sem)
    token_copy.start()

    to_y = seq_of(z, other_y, core)
    to_core = seq_of(z, y, other_core)
    has_up, has_down = z + 1 < depth, z > 0
    up = seq_of(lax.rem(z + 1, depth), y, core)
    down = seq_of(lax.rem(z + depth - 1, depth), y, core)

    barrier = pltpu.get_barrier_semaphore()

    def greet(group_at, seq_at):
        pl.semaphore_signal(
            barrier, inc=1, device_id={"group": group_at, "seq": seq_at}, device_id_type=MESH
        )

    for seq_at in (up, down, to_y, to_core):
        greet(group, seq_at)
    greet(other_group, me)
    for region in range(REGIONS):
        if region != REACH:
            greet(group, lax.rem(me + region - REACH + n, n))
    pl.semaphore_wait(barrier, 5 + REGIONS - 1)

    def to_partner(j, ref):
        copy_to(ref, cs.at[j], cr.at[j], group, to_core)

    def go(j, z_at, y_at, k, way):
        @pl.when(has_up if way == 0 else has_down)
        def _():
            copy_to(piece(j, z_at, y_at, group), zs.at[j, way, k], zr.at[j, y_at, z_at], group,
                    up if way == 0 else down)

    def begin(j):
        for part in (0, 1):
            loads[2 * j + part].wait()
        for part in (0, 1):
            copy_to(piece(j, z, y, part), ys.at[j], yr.at[j, part], group, to_y)
            to_partner(j, piece(j, z, y, part))
        go(j, z, y, 0, 0)
        go(j, z, y, 0, 1)

    def cross(j):
        for part in (0, 1):
            wait(piece(j, z, other_y, part), yr.at[j, part])
            to_partner(j, piece(j, z, other_y, part))
        go(j, z, other_y, 0, 0)
        go(j, z, other_y, 0, 1)

    def both(k, visit):
        @pl.when(z - k >= 0)
        def _():
            visit(z - k, 0)

        @pl.when(z + k < depth)
        def _():
            visit(z + k, 1)

    def along(j, k):
        def visit(zz, way):
            for y_at in (y, other_y):
                ref = piece(j, zz, y_at, group)
                wait(ref, zr.at[j, y_at, zz])
                go(j, zz, y_at, k, way)
                copy_to(ref, xs.at[j], xr.at[j, y_at, zz], other_group, me)
                to_partner(j, ref)

        both(k, visit)

    def finish(j, k):
        def visit(zz, way):
            for y_at in (y, other_y):
                ref = piece(j, zz, y_at, other_group)
                wait(ref, xr.at[j, y_at, zz])
                to_partner(j, ref)

        both(k, visit)

    work = Work(n, (gain, lengths, pages, freq, wide_gain, xbuf, onehot, cosine, sine), me)

    def project(j):
        wait(wbuf.at[j, :, :, other_core], cr.at[j])
        for at in range(0, width, TILE):
            def put(placed):
                pbuf[j, :, at : at + TILE] = placed

            weights = wbuf[j, :, :, :, :, :, at : at + TILE].reshape(work.features, TILE)
            work.project(weights, j < per_kind, put)

    def spot(j, region):
        rows = pl.ds(region * BLOCK, BLOCK)
        return (
            pbuf.at[j, rows, :],
            out.at[j // per_kind, rows, pl.ds((j % per_kind) * width, width)],
        )

    def hand_over(j):
        for region in range(REGIONS):
            src, dst = spot(j, region)
            if region == REACH:
                pltpu.make_async_copy(src, dst, hr.at[j, region]).start()
            else:
                copy_to(src, hs.at[j, region], hr.at[j, region], group,
                        lax.rem(me + region - REACH + n, n), dst)

    for j in range(chunks):
        begin(j)
    work.spread_gain()
    token_copy.wait()
    work.normalise(0, work.tok_rows)
    work.mark_rows()
    work.angles(0, work.tok_rows)
    for j in range(chunks):
        cross(j)
        lax.fori_loop(1, depth, lambda k, carry: (along(j, k), carry)[1], 0)
        lax.fori_loop(1, depth, lambda k, carry: (finish(j, k), carry)[1], 0)
        project(j)
        hand_over(j)

    for j in range(chunks):
        wait(wbuf.at[j, z, y, core], ys.at[j])
        wait(wbuf.at[j, 1:, :, core, group], xs.at[j])
        wait(wbuf.at[j, :, :, core], cs.at[j])
        sent = wbuf.at[j, 0, :, core, group]

        def drain(k, carry):
            @pl.when(has_up & (z - k >= 0))
            def _():
                wait(sent, zs.at[j, 0, k])

            @pl.when(has_down & (z + k < depth))
            def _():
                wait(sent, zs.at[j, 1, k])

            return carry

        lax.fori_loop(0, depth, drain, 0)
        for region in range(REGIONS):
            src, dst = spot(j, region)
            wait(dst, hr.at[j, region])
            if region != REACH:
                wait(src, hs.at[j, region])


def on_device(n, tokens, norm_gain, w_key, w_value, lengths, page_table):
    tok_rows, features = tokens.shape
    columns = w_key.shape[1]
    freq = ROPE_THETA ** (-(np.arange(HEAD // 2) * 2.0 / HEAD))
    freq = np.concatenate([freq, freq]).astype(np.float32)[None, :]
    depth = n // 4
    half = w_key.shape[0] // 2
    dma = pltpu.SemaphoreType.DMA
    vmem = pl.BlockSpec(memory_space=pltpu.VMEM)
    smem = pl.BlockSpec(memory_space=pltpu.SMEM)
    hbm = pl.BlockSpec(memory_space=pl.ANY)
    in_line = depth == LAYERS
    chunks = len(CHUNKS) if in_line else LOOP_CHUNKS
    groups = len(GROUPS) if in_line else chunks
    width = 2 * columns // chunks
    wide = width * max(GROUPS) if in_line else width
    scratch = [
        pltpu.VMEM((1, features), jnp.float32),
        pltpu.VMEM((chunks, depth, 2, 2, 2, half, width), jnp.bfloat16),
        pltpu.VMEM((tok_rows, features), jnp.bfloat16),
        pltpu.VMEM((groups, ROWS, wide), jnp.bfloat16),
    ]
    if in_line:
        scratch.append(pltpu.VMEM((max(len(RELAYED), 1), 2, BLOCK, wide), jnp.bfloat16))
    scratch += [
        pltpu.VMEM((ROWS, tok_rows), jnp.bfloat16),
        pltpu.VMEM((tok_rows, HEAD), jnp.float32),
        pltpu.VMEM((tok_rows, HEAD), jnp.float32),
        dma((chunks, 2)),
        dma,
    ]
    each, by_layer, by_region = dma((chunks,)), dma((chunks, depth)), dma((groups, REGIONS))
    if in_line:
        slots = dma((groups, 2))
        scratch += [each, each, by_layer, by_layer, each, each, by_layer, each, each, by_layer, by_layer,
                    each, each, by_region, by_region, slots, slots]
    else:
        by_line = dma((chunks, 2, depth))
        scratch += [each, dma((chunks, 2)), by_line, by_line, each, by_line, each, each,
                    by_region, by_region]
    cache = pl.pallas_call(
        functools.partial(line_kernel if in_line else loop_kernel, n),
        out_shape=jax.ShapeDtypeStruct((2, ROWS, columns), jnp.bfloat16),
        in_specs=[hbm, vmem, hbm, hbm, smem, vmem, vmem],
        out_specs=hbm,
        scratch_shapes=scratch,
        compiler_params=pltpu.CompilerParams(
            collective_id=0, has_side_effects=True, vmem_limit_bytes=60 * 2**20
        ),
    )(tokens, norm_gain.reshape(-1, HEAD), w_key, w_value, lengths, page_table[None, :], freq)
    return cache.reshape(2, SLOTS, PAGE, columns)


def solution(mesh):
    placed = (
        P(("group", "seq"), None),
        P(),
        P("seq", None),
        P("seq", None),
        P("group"),
        P(("group", "seq")),
    )
    return jax.shard_map(
        functools.partial(on_device, mesh.shape["seq"]),
        mesh=mesh,
        in_specs=placed,
        out_specs=P(None, ("group", "seq"), None, None),
        check_vma=False,
    )
```

```python
import functools

import jax
import jax.numpy as jnp
import numpy as np
from jax import lax
from jax.experimental import pallas as pl
from jax.experimental.pallas import tpu as pltpu
from jax.sharding import PartitionSpec as P

HEAD = 128
PAGE = 16
REACH = 2
CAP = 8
SLOTS = 40
REGIONS = 2 * REACH + 1
BLOCK = CAP * PAGE
ROWS = SLOTS * PAGE

ROPE_THETA = 500000.0
EPS = 1e-05

TILE = 256
MESH = pl.DeviceIdType.MESH

PAIRED, SPLIT, TURNED = 0, 1, 2
CHUNKS = ((SPLIT, True), (PAIRED, False), (PAIRED, True), (SPLIT, True), (PAIRED, True), (SPLIT, True), (PAIRED, True), (PAIRED, True))
GROUPS = (1, 1, 1, 1, 1, 1, 1, 1)
RELAYED = (1, 5)

LAYERS = 4
LOOP_CHUNKS = 8

BEGIN, CROSS, ACROSS, ALONG, FACE, SIDE, SETTLE, UP, DOWN, RELAY = range(10)
COMPUTE = (0,0,0,0,0,0,0,0,0,0,0,0,0,0,0,0,0,0,0,0,1,1,1,1,1,1,1,1)
END_FIRST = (
    ((BEGIN, 0, 0, 0), (BEGIN, 0, 0, 1),),
    (),
    (),
    ((BEGIN, 1, 0, 0),),
    (),
    (),
    ((BEGIN, 1, 0, 1),),
    (),
    (),
    (),
    (),
    (),
    (),
    (),
    ((BEGIN, 2, 0, 0),),
    (),
    (),
    ((ALONG, 0, 1, -1), (ALONG, 0, 1, 0), (ALONG, 0, 1, 1),),
    (),
    ((CROSS, 0, 0, -1), (CROSS, 0, 0, 0), (CROSS, 0, 0, 1),),
    ((CROSS, 1, 0, -1), (CROSS, 1, 0, 0), (CROSS, 1, 0, 1), (FACE, 0, 1, -1), (FACE, 0, 1, 0), (BEGIN, 3, 0, 0),
     (ALONG, 3, 1, -1), (ALONG, 3, 1, 0), (ACROSS, 1, 0, -1), (ACROSS, 1, 0, 0), (ACROSS, 1, 0, 1),
     (ALONG, 1, 1, -1), (ALONG, 1, 1, 0), (BEGIN, 2, 0, 1), (CROSS, 2, 0, -1), (CROSS, 2, 0, 1),
     (SETTLE, 0, 1, -1), (SETTLE, 0, 1, 0), (ALONG, 2, 1, -1), (ALONG, 2, 1, 0), (ALONG, 3, 1, 1),
     (ALONG, 0, 2, -1), (ALONG, 0, 2, 1), (CROSS, 2, 0, 0), (FACE, 1, 1, -1), (FACE, 1, 1, 0), (FACE, 3, 1, -1),
     (FACE, 3, 1, 0), (ALONG, 0, 2, 0), (ALONG, 1, 2, -1), (ALONG, 1, 2, 0), (CROSS, 3, 0, -1),
     (CROSS, 3, 0, 1), (BEGIN, 4, 0, 0), (BEGIN, 3, 0, 1), (ALONG, 2, 2, -1), (FACE, 2, 1, -1),
     (FACE, 2, 1, 0), (SETTLE, 3, 1, -1), (SETTLE, 3, 1, 0), (ALONG, 2, 2, 0), (ALONG, 3, 2, -1),
     (FACE, 0, 2, -1), (FACE, 0, 2, 0), (CROSS, 3, 0, 0), (ALONG, 0, 3, -1), (ALONG, 3, 2, 1), (ALONG, 0, 3, 1),
     (FACE, 1, 2, -1), (FACE, 1, 2, 0), (ALONG, 0, 3, 0), (CROSS, 4, 0, -1), (CROSS, 4, 0, 1), (BEGIN, 4, 0, 1),
     (BEGIN, 5, 0, 0), (ALONG, 3, 2, 0), (CROSS, 4, 0, 0), (FACE, 2, 2, -1), (FACE, 2, 2, 0), (SETTLE, 0, 2, -1),
     (SETTLE, 0, 2, 0), (FACE, 0, 3, -1), (FACE, 0, 3, 0), (BEGIN, 5, 0, 1), (ALONG, 1, 3, -1),
     (ALONG, 1, 3, 0), (FACE, 3, 2, -1), (FACE, 3, 2, 0), (ALONG, 4, 1, -1), (ALONG, 4, 1, 0), (BEGIN, 6, 0, 0),
     (CROSS, 5, 0, -1), (CROSS, 5, 0, 1), (ALONG, 4, 2, -1), (ALONG, 4, 2, 0), (CROSS, 5, 0, 0),
     (BEGIN, 7, 0, 0), (SETTLE, 0, 3, -1), (SETTLE, 0, 3, 0), (FACE, 1, 3, -1), (FACE, 1, 3, 0),
     (BEGIN, 6, 0, 1), (ALONG, 2, 3, -1), (ALONG, 2, 3, 0), (ALONG, 5, 2, -1),),
    (),
    ((SETTLE, 3, 2, -1), (SETTLE, 3, 2, 0), (ALONG, 5, 1, -1), (ALONG, 5, 1, 1), (FACE, 4, 1, -1),
     (FACE, 4, 1, 0), (ALONG, 5, 2, 1), (ALONG, 3, 3, -1), (ALONG, 3, 3, 1), (ALONG, 3, 3, 0), (ALONG, 5, 1, 0),
     (CROSS, 6, 0, -1), (CROSS, 6, 0, 1), (CROSS, 6, 0, 0), (FACE, 4, 2, -1), (FACE, 4, 2, 0), (CROSS, 7, 0, -1),
     (CROSS, 7, 0, 1), (ALONG, 5, 2, 0), (BEGIN, 7, 0, 1), (FACE, 2, 3, -1), (FACE, 2, 3, 0), (ALONG, 6, 1, -1),
     (ALONG, 6, 1, 0), (DOWN, 0, 0, 0), (FACE, 3, 3, -1), (FACE, 3, 3, 0), (UP, 0, 0, 0),),
    ((ALONG, 4, 3, -1), (UP, 0, 0, 1), (CROSS, 7, 0, 0), (ALONG, 4, 3, 0), (FACE, 5, 1, -1), (FACE, 5, 1, 0),
     (FACE, 5, 2, -1), (FACE, 5, 2, 0), (SETTLE, 5, 1, -1), (SETTLE, 5, 1, 0), (DOWN, 0, 0, 1),
     (SETTLE, 3, 3, -1), (SETTLE, 3, 3, 0), (ALONG, 6, 2, -1), (UP, 1, 0, 0), (FACE, 6, 1, -1),
     (FACE, 6, 1, 0), (ALONG, 5, 3, -1), (ALONG, 5, 3, 0), (ALONG, 5, 3, 1), (ALONG, 6, 2, 0), (DOWN, 2, 0, 0),
     (UP, 2, 0, 0), (FACE, 5, 3, -1), (FACE, 5, 3, 0), (FACE, 4, 3, -1), (FACE, 4, 3, 0), (DOWN, 1, 0, 1),
     (SETTLE, 5, 2, -1), (SETTLE, 5, 2, 0), (ALONG, 7, 1, -1), (ALONG, 7, 1, 0), (UP, 1, 0, 1),
     (DOWN, 2, 0, 1), (UP, 2, 0, 1),),
    ((UP, 3, 0, 0), (DOWN, 1, 0, 0),),
    ((DOWN, 3, 0, 1), (UP, 3, 0, 1), (UP, 4, 0, 0), (FACE, 6, 2, -1), (FACE, 6, 2, 0), (ALONG, 6, 3, -1),
     (ALONG, 6, 3, 0), (DOWN, 3, 0, 0), (ALONG, 7, 2, -1), (ALONG, 7, 2, 0), (DOWN, 4, 0, 0), (SETTLE, 5, 3, -1),
     (SETTLE, 5, 3, 0), (DOWN, 4, 0, 1), (UP, 4, 0, 1), (FACE, 7, 1, -1), (FACE, 7, 1, 0),),
    ((UP, 5, 0, 0), (DOWN, 5, 0, 0), (ALONG, 7, 3, -1), (ALONG, 7, 3, 0), (UP, 5, 0, 1), (DOWN, 5, 0, 1),
     (FACE, 6, 3, -1), (FACE, 6, 3, 0), (FACE, 7, 2, -1), (FACE, 7, 2, 0),),
    ((DOWN, 6, 0, 0), (UP, 6, 0, 0), (UP, 6, 0, 1), (DOWN, 6, 0, 1), (FACE, 7, 3, -1), (FACE, 7, 3, 0),
     ),
    ((DOWN, 7, 0, 0), (DOWN, 7, 0, 1), (UP, 7, 0, 0), (UP, 7, 0, 1),),
)
END_SECOND = (
    ((BEGIN, 0, 0, 0), (BEGIN, 0, 0, 1),),
    (),
    (),
    (),
    ((BEGIN, 1, 0, 0),),
    ((BEGIN, 1, 0, 1),),
    (),
    (),
    (),
    (),
    (),
    (),
    (),
    (),
    (),
    ((BEGIN, 2, 0, 0),),
    (),
    (),
    ((ALONG, 0, 1, -1), (ALONG, 0, 1, 0), (ALONG, 0, 1, 1),),
    (),
    ((CROSS, 0, 0, -1), (CROSS, 0, 0, 0), (CROSS, 0, 0, 1), (CROSS, 1, 0, -1), (CROSS, 1, 0, 0),
     (CROSS, 1, 0, 1), (ALONG, 3, 1, -1), (ALONG, 3, 1, 0), (FACE, 0, 1, -1), (FACE, 0, 1, 0), (BEGIN, 3, 0, 0),
     (ACROSS, 1, 0, -1), (ACROSS, 1, 0, 0), (ACROSS, 1, 0, 1), (ALONG, 1, 1, -1), (ALONG, 1, 1, 0),
     (FACE, 3, 1, -1), (FACE, 3, 1, 0), (BEGIN, 2, 0, 1), (CROSS, 2, 0, -1), (CROSS, 2, 0, 1), (ALONG, 2, 1, -1),
     (ALONG, 2, 1, 0), (ALONG, 3, 1, 1), (SETTLE, 0, 1, -1), (SETTLE, 0, 1, 0), (CROSS, 2, 0, 0),
     (FACE, 1, 1, -1), (FACE, 1, 1, 0), (ALONG, 0, 2, -1), (ALONG, 0, 2, 1), (ALONG, 0, 2, 0), (BEGIN, 4, 0, 0),
     (CROSS, 3, 0, -1), (CROSS, 3, 0, 1), (CROSS, 3, 0, 0), (BEGIN, 3, 0, 1), (ALONG, 1, 2, -1),
     (ALONG, 1, 2, 0), (FACE, 2, 1, -1), (FACE, 2, 1, 0), (ALONG, 2, 2, -1), (ALONG, 2, 2, 0), (SETTLE, 3, 1, -1),
     (SETTLE, 3, 1, 0), (FACE, 0, 2, -1), (FACE, 0, 2, 0), (ALONG, 3, 2, -1), (ALONG, 0, 3, -1),
     (ALONG, 0, 3, 0), (ALONG, 0, 3, 1), (FACE, 1, 2, -1), (FACE, 1, 2, 0), (ALONG, 3, 2, 1), (BEGIN, 4, 0, 1),
     (ALONG, 3, 2, 0), (ALONG, 4, 1, -1), (ALONG, 4, 1, 0), (BEGIN, 5, 0, 0), (CROSS, 4, 0, -1),
     (CROSS, 4, 0, 0), (CROSS, 4, 0, 1), (SETTLE, 0, 2, -1), (SETTLE, 0, 2, 0), (FACE, 2, 2, -1),
     (FACE, 2, 2, 0), (ALONG, 1, 3, -1), (ALONG, 1, 3, 0), (BEGIN, 5, 0, 1), (FACE, 0, 3, -1), (FACE, 0, 3, 0),
     (FACE, 3, 2, -1), (FACE, 3, 2, 0), (BEGIN, 6, 0, 0), (CROSS, 5, 0, -1), (CROSS, 5, 0, 0), (CROSS, 5, 0, 1),
     (ALONG, 4, 2, -1), (ALONG, 4, 2, 0), (SETTLE, 0, 3, -1), (SETTLE, 0, 3, 0), (FACE, 1, 3, -1),
     (FACE, 1, 3, 0), (FACE, 4, 1, -1), (FACE, 4, 1, 0), (SETTLE, 3, 2, -1), (SETTLE, 3, 2, 0),
     (BEGIN, 7, 0, 0), (ALONG, 2, 3, -1), (ALONG, 2, 3, 0), (ALONG, 5, 2, -1), (ALONG, 5, 2, 1),
     (BEGIN, 6, 0, 1),),
    (),
    ((ALONG, 5, 1, -1), (ALONG, 5, 1, 1), (ALONG, 5, 2, 0), (ALONG, 3, 3, -1), (ALONG, 3, 3, 0),
     (ALONG, 3, 3, 1), (ALONG, 5, 1, 0), (CROSS, 6, 0, -1), (CROSS, 6, 0, 0), (CROSS, 6, 0, 1),
     (FACE, 4, 2, -1), (FACE, 4, 2, 0), (BEGIN, 7, 0, 1), (FACE, 2, 3, -1), (FACE, 2, 3, 0), (CROSS, 7, 0, -1),
     (CROSS, 7, 0, 1), (ALONG, 6, 1, -1), (ALONG, 6, 1, 0), (DOWN, 0, 0, 0), (UP, 0, 0, 0), (UP, 1, 0, 1),
     (CROSS, 7, 0, 0), (FACE, 3, 3, -1), (FACE, 3, 3, 0), (ALONG, 4, 3, -1), (ALONG, 4, 3, 0), (FACE, 5, 1, -1),
     (FACE, 5, 1, 0), (FACE, 5, 2, -1), (FACE, 5, 2, 0), (SETTLE, 3, 3, -1), (SETTLE, 3, 3, 0),
     (DOWN, 0, 0, 1), (UP, 0, 0, 1),),
    ((DOWN, 1, 0, 0), (UP, 1, 0, 0), (ALONG, 5, 3, -1), (ALONG, 5, 3, 0), (ALONG, 5, 3, 1), (FACE, 6, 1, -1),
     (FACE, 6, 1, 0), (ALONG, 6, 2, -1), (ALONG, 6, 2, 0), (DOWN, 1, 0, 1), (SETTLE, 5, 1, -1),
     (SETTLE, 5, 1, 0), (DOWN, 2, 0, 0), (UP, 2, 0, 0),),
    ((FACE, 4, 3, -1), (FACE, 4, 3, 0), (SETTLE, 5, 2, -1), (SETTLE, 5, 2, 0), (DOWN, 2, 0, 1),
     (FACE, 5, 3, -1), (FACE, 5, 3, 0), (ALONG, 7, 1, -1), (ALONG, 7, 1, 0), (UP, 3, 0, 0), (UP, 2, 0, 1),
     ),
    ((DOWN, 3, 0, 1), (UP, 3, 0, 1), (FACE, 6, 2, -1), (FACE, 6, 2, 0), (ALONG, 6, 3, -1), (ALONG, 6, 3, 0),
     (UP, 4, 0, 0), (DOWN, 3, 0, 0), (DOWN, 4, 0, 0), (SETTLE, 5, 3, -1), (SETTLE, 5, 3, 0), (UP, 4, 0, 1),
     (DOWN, 4, 0, 1), (FACE, 7, 1, -1), (FACE, 7, 1, 0),),
    ((DOWN, 5, 0, 0), (UP, 5, 0, 0), (UP, 5, 0, 1), (DOWN, 5, 0, 1), (ALONG, 7, 2, -1), (ALONG, 7, 2, 0),
     (FACE, 6, 3, -1), (FACE, 6, 3, 0),),
    ((UP, 6, 0, 0), (DOWN, 6, 0, 0), (ALONG, 7, 3, -1), (ALONG, 7, 3, 0), (UP, 6, 0, 1), (DOWN, 6, 0, 1),
     (FACE, 7, 2, -1), (FACE, 7, 2, 0), (FACE, 7, 3, -1), (FACE, 7, 3, 0),),
    ((DOWN, 7, 0, 0), (UP, 7, 0, 0), (DOWN, 7, 0, 1), (UP, 7, 0, 1),),
)
INNER_FIRST = (
    ((BEGIN, 0, 0, 0), (BEGIN, 0, 0, 1), (BEGIN, 0, 0, 2), (BEGIN, 1, 0, 0),),
    (),
    ((BEGIN, 1, 0, 2), (BEGIN, 1, 0, 1),),
    ((BEGIN, 2, 0, 0),),
    (),
    (),
    ((BEGIN, 2, 0, 2),),
    ((BEGIN, 2, 0, 1),),
    ((BEGIN, 3, 0, 1),),
    (),
    ((BEGIN, 3, 0, 0),),
    (),
    (),
    ((CROSS, 0, 0, -1), (CROSS, 0, 0, 0), (CROSS, 0, 0, 1),),
    (),
    ((BEGIN, 4, 0, 0),),
    (),
    ((CROSS, 1, 0, -1), (CROSS, 1, 0, 0), (CROSS, 1, 0, 1), (CROSS, 1, 0, 2),),
    (),
    ((BEGIN, 5, 0, 0),),
    ((CROSS, 2, 0, -1), (CROSS, 2, 0, 0), (CROSS, 2, 0, 2), (CROSS, 2, 0, 1), (ACROSS, 0, 0, -1),
     (ACROSS, 0, 0, 0), (CROSS, 3, 0, -1), (CROSS, 3, 0, 0), (CROSS, 3, 0, 1), (BEGIN, 6, 0, 0),
     (BEGIN, 3, 0, 2), (ALONG, 0, 2, -1), (ALONG, 0, 2, 0), (ALONG, 0, 2, 1), (BEGIN, 7, 0, 0),
     (ACROSS, 1, 0, -1), (ACROSS, 1, 0, 0), (CROSS, 4, 0, -1), (ALONG, 1, 2, -1), (ALONG, 1, 2, 0),
     (ALONG, 1, 2, 1), (ACROSS, 2, 0, -1), (ACROSS, 2, 0, 0), (ALONG, 0, 0, -1), (ALONG, 0, 0, 0),
     (ALONG, 0, 0, 1), (ALONG, 2, 2, -1), (ALONG, 2, 2, 0), (CROSS, 5, 0, -1), (ALONG, 2, 2, 1),
     (CROSS, 6, 0, -1), (ACROSS, 3, 0, -1), (ACROSS, 3, 0, 0), (ALONG, 3, 2, -1), (ALONG, 1, 0, -1),
     (ALONG, 1, 0, 0), (ALONG, 1, 0, 1), (CROSS, 4, 0, 0), (FACE, 0, 2, -1), (FACE, 0, 2, 0), (CROSS, 7, 0, -1),
     (ALONG, 3, 2, 0), (ALONG, 0, 3, -1), (ALONG, 0, 3, 0), (BEGIN, 4, 0, 2), (ALONG, 0, 3, 1),
     (BEGIN, 4, 0, 1), (FACE, 1, 2, -1), (FACE, 1, 2, 0), (ALONG, 2, 0, -1), (ALONG, 2, 0, 0), (ALONG, 2, 0, 1),
     (CROSS, 4, 0, 1), (FACE, 2, 2, -1), (FACE, 2, 2, 0), (ALONG, 1, 3, -1), (ALONG, 1, 3, 0), (ALONG, 1, 3, 1),
     (ALONG, 3, 2, 1), (CROSS, 5, 0, 0), (CROSS, 4, 0, 2), (BEGIN, 5, 0, 2), (FACE, 0, 3, -1), (FACE, 0, 3, 0),
     (ALONG, 4, 2, -1), (ALONG, 4, 2, 0), (FACE, 1, 3, -1), (FACE, 1, 3, 0), (BEGIN, 6, 0, 2), (ALONG, 3, 0, -1),
     (ALONG, 3, 0, 0), (ALONG, 3, 0, 1), (ALONG, 2, 3, -1), (ALONG, 2, 3, 0), (ALONG, 2, 3, 1),
     (CROSS, 6, 0, 0), (ALONG, 4, 2, 1), (BEGIN, 5, 0, 1),),
    ((FACE, 3, 2, -1), (FACE, 3, 2, 0), (ALONG, 5, 2, -1), (ALONG, 5, 2, 0),),
    ((UP, 1, 0, 1), (BEGIN, 6, 0, 1), (ALONG, 4, 0, -1), (ALONG, 4, 0, 0), (ALONG, 4, 0, 1), (ACROSS, 4, 0, -1),
     (ACROSS, 4, 0, 0), (ALONG, 3, 3, -1), (ALONG, 3, 3, 0), (ALONG, 3, 3, 1), (UP, 1, 0, 0), (FACE, 2, 3, -1),
     (FACE, 2, 3, 0), (ALONG, 6, 2, -1), (CROSS, 7, 0, 0), (BEGIN, 7, 0, 2), (DOWN, 1, 0, 0), (CROSS, 6, 0, 1),
     (CROSS, 5, 0, 1),),
    ((DOWN, 1, 0, 1), (ALONG, 5, 0, -1), (ALONG, 5, 0, 0), (ALONG, 5, 0, 1), (FACE, 4, 2, -1), (FACE, 4, 2, 0),
     (ALONG, 6, 2, 0), (ALONG, 4, 3, -1), (ALONG, 4, 3, 0), (ALONG, 4, 3, 1), (FACE, 3, 3, -1),
     (FACE, 3, 3, 0), (ALONG, 5, 2, 1), (ALONG, 7, 2, -1),),
    ((ACROSS, 5, 0, -1), (ACROSS, 5, 0, 0), (UP, 0, 0, 0), (DOWN, 0, 0, 0), (ALONG, 6, 0, -1), (ALONG, 6, 0, 0),
     (ALONG, 6, 0, 1), (FACE, 4, 3, -1), (FACE, 4, 3, 0), (CROSS, 7, 0, 1), (ALONG, 5, 3, -1), (ALONG, 5, 3, 0),
     (ALONG, 5, 3, 1), (CROSS, 6, 0, 2), (BEGIN, 7, 0, 1), (UP, 0, 0, 1), (DOWN, 0, 0, 1), (ALONG, 6, 2, 1),
     (ALONG, 7, 2, 0), (FACE, 5, 2, -1), (FACE, 5, 2, 0), (ALONG, 6, 3, -1), (ALONG, 6, 3, 0), (ALONG, 7, 0, -1),
     (ALONG, 7, 0, 0), (ALONG, 7, 0, 1), (UP, 2, 0, 0), (FACE, 5, 3, -1), (FACE, 5, 3, 0), (DOWN, 2, 0, 0),
     (CROSS, 7, 0, 2), (ALONG, 6, 3, 1), (ACROSS, 6, 0, -1), (ACROSS, 6, 0, 0), (UP, 2, 0, 1), (DOWN, 2, 0, 1),
     (UP, 3, 0, 0), (ALONG, 7, 2, 1), (FACE, 6, 2, -1), (FACE, 6, 2, 0), (ALONG, 7, 3, -1), (ALONG, 7, 3, 0),
     (UP, 3, 0, 1), (DOWN, 3, 0, 1), (DOWN, 3, 0, 0), (FACE, 6, 3, -1), (FACE, 6, 3, 0), (ALONG, 7, 3, 1),
     ),
    ((UP, 4, 0, 0),),
    ((DOWN, 5, 0, 0), (UP, 5, 0, 0), (UP, 5, 0, 1), (ACROSS, 7, 0, -1), (ACROSS, 7, 0, 0), (DOWN, 5, 0, 1),
     ),
    ((DOWN, 4, 0, 1), (UP, 4, 0, 1), (DOWN, 4, 0, 0), (FACE, 7, 3, -1), (FACE, 7, 3, 0), (FACE, 7, 2, -1),
     (FACE, 7, 2, 0), (RELAY, 1, 0, 0), (DOWN, 6, 0, 0),),
    ((UP, 6, 0, 1), (DOWN, 6, 0, 1), (UP, 6, 0, 0), (DOWN, 7, 0, 0), (UP, 7, 0, 0), (DOWN, 7, 0, 1),
     (RELAY, 5, 0, 0), (UP, 7, 0, 1),),
)
INNER_SECOND = (
    ((BEGIN, 0, 0, 0), (BEGIN, 0, 0, 1), (BEGIN, 0, 0, 2), (BEGIN, 1, 0, 0),),
    ((BEGIN, 1, 0, 1), (BEGIN, 1, 0, 2),),
    (),
    ((BEGIN, 2, 0, 0),),
    ((BEGIN, 2, 0, 2),),
    (),
    (),
    ((BEGIN, 2, 0, 1),),
    (),
    ((BEGIN, 3, 0, 1),),
    (),
    ((BEGIN, 3, 0, 0), (BEGIN, 4, 0, 0),),
    ((CROSS, 0, 0, -1), (CROSS, 0, 0, 0), (CROSS, 0, 0, 1),),
    (),
    (),
    (),
    ((CROSS, 1, 0, -1), (CROSS, 1, 0, 0), (CROSS, 1, 0, 1), (CROSS, 1, 0, 2),),
    (),
    (),
    ((BEGIN, 5, 0, 0),),
    ((CROSS, 2, 0, -1), (CROSS, 2, 0, 0), (CROSS, 2, 0, 2), (CROSS, 2, 0, 1), (BEGIN, 3, 0, 2),
     (CROSS, 3, 0, -1), (CROSS, 3, 0, 1), (ALONG, 0, 2, -1), (ALONG, 0, 2, 0), (ALONG, 0, 2, 1),
     (CROSS, 3, 0, 0), (ACROSS, 0, 0, -1), (ACROSS, 0, 0, 0), (BEGIN, 7, 0, 0), (CROSS, 4, 0, -1),
     (ALONG, 1, 2, -1), (ALONG, 1, 2, 0), (ALONG, 1, 2, 1), (ALONG, 2, 2, -1), (CROSS, 5, 0, -1),
     (ALONG, 0, 0, -1), (ALONG, 0, 0, 0), (ALONG, 0, 0, 1), (ALONG, 2, 2, 0), (ACROSS, 1, 0, -1),
     (ACROSS, 1, 0, 0), (ACROSS, 2, 0, -1), (ACROSS, 2, 0, 0), (BEGIN, 6, 0, 0), (CROSS, 6, 0, -1),
     (ALONG, 3, 2, -1), (ALONG, 2, 2, 1), (FACE, 0, 2, -1), (FACE, 0, 2, 0), (ALONG, 1, 0, -1),
     (ALONG, 1, 0, 0), (ALONG, 1, 0, 1), (CROSS, 7, 0, -1), (ACROSS, 3, 0, -1), (ACROSS, 3, 0, 0),
     (ALONG, 3, 2, 0), (BEGIN, 4, 0, 2), (ALONG, 0, 3, -1), (ALONG, 0, 3, 0), (BEGIN, 4, 0, 1),
     (ALONG, 0, 3, 1), (CROSS, 4, 0, 0), (FACE, 1, 2, -1), (FACE, 1, 2, 0), (ALONG, 2, 0, -1), (ALONG, 2, 0, 0),
     (ALONG, 2, 0, 1), (CROSS, 4, 0, 1), (ALONG, 1, 3, -1), (ALONG, 1, 3, 0), (FACE, 2, 2, -1),
     (FACE, 2, 2, 0), (ALONG, 1, 3, 1), (ALONG, 3, 2, 1), (BEGIN, 5, 0, 2), (ALONG, 4, 2, -1), (FACE, 0, 3, -1),
     (FACE, 0, 3, 0), (ALONG, 4, 2, 0), (CROSS, 5, 0, 0), (CROSS, 4, 0, 2), (BEGIN, 6, 0, 2), (ALONG, 3, 0, -1),
     (ALONG, 3, 0, 0), (ALONG, 3, 0, 1), (ALONG, 2, 3, -1), (ALONG, 2, 3, 0), (ALONG, 2, 3, 1),
     (FACE, 1, 3, -1), (FACE, 1, 3, 0), (ALONG, 4, 2, 1), (BEGIN, 5, 0, 1),),
    ((ALONG, 5, 2, -1), (FACE, 3, 2, -1), (FACE, 3, 2, 0), (CROSS, 6, 0, 0), (ALONG, 5, 2, 0), (DOWN, 0, 0, 0),
     (BEGIN, 6, 0, 1), (ALONG, 4, 0, -1), (ALONG, 4, 0, 0), (ALONG, 4, 0, 1),),
    ((ALONG, 3, 3, -1), (ALONG, 3, 3, 0), (ALONG, 3, 3, 1), (FACE, 2, 3, -1), (FACE, 2, 3, 0), (ACROSS, 4, 0, -1),
     (ACROSS, 4, 0, 0), (BEGIN, 7, 0, 2), (UP, 0, 0, 0), (CROSS, 5, 0, 1), (ALONG, 6, 2, -1), (CROSS, 6, 0, 1),
     (CROSS, 7, 0, 0),),
    ((DOWN, 0, 0, 1), (FACE, 4, 2, -1), (FACE, 4, 2, 0), (ALONG, 5, 0, -1), (ALONG, 5, 0, 0), (ALONG, 5, 0, 1),
     (ALONG, 4, 3, -1), (ALONG, 4, 3, 0), (ALONG, 4, 3, 1), (RELAY, 1, 0, 0), (DOWN, 1, 0, 0), (ALONG, 5, 2, 1),
     (UP, 0, 0, 1), (FACE, 3, 3, -1), (FACE, 3, 3, 0), (UP, 1, 0, 0), (UP, 1, 0, 1), (ALONG, 6, 2, 0),
     (ALONG, 7, 2, -1), (DOWN, 1, 0, 1),),
    ((UP, 2, 0, 0), (ALONG, 6, 0, -1), (ALONG, 6, 0, 0), (ALONG, 6, 0, 1), (DOWN, 2, 0, 0), (ALONG, 5, 3, -1),
     (ALONG, 5, 3, 0), (CROSS, 7, 0, 1), (ACROSS, 5, 0, -1), (ACROSS, 5, 0, 0), (FACE, 4, 3, -1),
     (FACE, 4, 3, 0), (ALONG, 5, 3, 1), (BEGIN, 7, 0, 1),),
    ((UP, 2, 0, 1), (ALONG, 6, 2, 1), (CROSS, 6, 0, 2), (DOWN, 2, 0, 1), (DOWN, 4, 0, 0), (FACE, 5, 2, -1),
     (FACE, 5, 2, 0), (DOWN, 3, 0, 1), (UP, 3, 0, 1), (UP, 3, 0, 0), (ALONG, 6, 3, -1), (ALONG, 6, 3, 0),
     (ALONG, 7, 0, -1), (ALONG, 7, 0, 0), (ALONG, 7, 0, 1), (FACE, 5, 3, -1), (FACE, 5, 3, 0), (ALONG, 7, 2, 0),
     (UP, 4, 0, 0), (ALONG, 6, 3, 1), (DOWN, 3, 0, 0), (ACROSS, 6, 0, -1), (ACROSS, 6, 0, 0), (ALONG, 7, 2, 1),
     (CROSS, 7, 0, 2), (UP, 4, 0, 1), (DOWN, 4, 0, 1), (FACE, 6, 2, -1), (FACE, 6, 2, 0), (FACE, 6, 3, -1),
     (FACE, 6, 3, 0), (ALONG, 7, 3, -1), (ALONG, 7, 3, 0), (ACROSS, 7, 0, -1), (ACROSS, 7, 0, 0),
     (FACE, 7, 2, -1), (FACE, 7, 2, 0), (ALONG, 7, 3, 1),),
    ((DOWN, 5, 0, 0), (DOWN, 5, 0, 1), (UP, 5, 0, 0), (UP, 5, 0, 1),),
    ((UP, 6, 0, 0), (RELAY, 5, 0, 0), (UP, 6, 0, 1), (DOWN, 6, 0, 1), (FACE, 7, 3, -1), (FACE, 7, 3, 0),
     (DOWN, 6, 0, 0),),
    ((DOWN, 7, 0, 0), (UP, 7, 0, 0), (DOWN, 7, 0, 1), (UP, 7, 0, 1),),
)


class Work:
    def __init__(self, n, refs, me):
        (self.gain, self.lengths, self.pages, self.freq, self.wide_gain, self.xbuf, self.raw, self.found,
         self.page_of, self.found_sem, self.cosine, self.sine) = refs
        self.n, self.me = n, me
        self.tok_rows, self.features = self.xbuf.shape
        self.length_each = self.tok_rows * n // 2
        self.first = lax.rem(me * self.tok_rows, self.length_each)

    def spread_gain(self):
        each = self.gain[...].astype(jnp.float32)
        rows = [each[i : i + 1, :] for i in range(self.features // HEAD)]
        self.wide_gain[...] = jnp.concatenate(rows, axis=1)

    def normalise(self, at, rows_here):
        xbuf = self.xbuf

        def body(i, carry):
            rows = pl.ds(pl.multiple_of(at + i * 32, 32), 32)
            wide = xbuf[rows, :].astype(jnp.float32)
            scale = lax.rsqrt(jnp.mean(wide * wide, axis=1, keepdims=True) + EPS)
            xbuf[rows, :] = (wide * scale * self.wide_gain[...]).astype(jnp.bfloat16)
            return carry

        lax.fori_loop(0, rows_here // 32, body, 0)

    def find_pages(self):
        page_count = self.tok_rows // PAGE
        lane = lax.broadcasted_iota(jnp.int32, self.found.shape, 1)
        page_of = jnp.full(self.found.shape, page_count, jnp.int32)
        for page in range(page_count):
            page_of = jnp.where(lane == lax.rem(self.pages[page], SLOTS), page, page_of)
        self.found[...] = page_of
        self.raw[page_count] = jnp.zeros(self.raw.shape[1:], jnp.bfloat16)
        copy = pltpu.make_async_copy(self.found, self.page_of, self.found_sem)
        copy.start()
        copy.wait()

    def angles(self, at, rows_here):
        def turn(i, carry):
            row_at = pl.multiple_of(at + i * 64, 64)
            row = lax.broadcasted_iota(jnp.int32, (64, HEAD), 0) + (self.first + row_at)
            lane = lax.broadcasted_iota(jnp.int32, (64, HEAD), 1)
            angle = row.astype(jnp.float32) * self.freq[...]
            self.cosine[pl.ds(row_at, 64), :] = jnp.cos(angle)
            sined = jnp.sin(angle)
            self.sine[pl.ds(row_at, 64), :] = jnp.where(lane < HEAD // 2, -sined, sined)
            return carry

        lax.fori_loop(0, rows_here // 64, turn, 0)

    def project(self, weights, is_key, put):
        part = self.tok_rows // 2
        raw = [
            jnp.dot(self.xbuf[i * part : (i + 1) * part, :], weights, preferred_element_type=jnp.float32)
            for i in range(2)
        ]
        raw = jnp.concatenate(raw, axis=0)
        if is_key:
            heads = []
            for head in range(weights.shape[1] // HEAD):
                one = raw[:, head * HEAD : (head + 1) * HEAD]
                heads.append(one * self.cosine[...] + pltpu.roll(one, HEAD // 2, 1) * self.sine[...])
            raw = jnp.concatenate(heads, axis=1)
        second_prompt = (self.me * self.tok_rows) // self.length_each
        limit = self.lengths[0] + second_prompt * (self.lengths[1] - self.lengths[0])
        row = lax.broadcasted_iota(jnp.int32, raw.shape, 0)
        raw = jnp.where(self.first + row < limit, raw, 0.0)
        wide = weights.shape[1]
        raw = raw.astype(jnp.bfloat16).reshape(self.tok_rows // PAGE, PAGE, wide)
        self.raw[0 : self.tok_rows // PAGE, :, 0:wide] = raw
        for slot in range(SLOTS):
            put(slot * PAGE, self.raw[self.page_of[0, slot]][:, 0:wide])


def copy_to(ref, send_sem, recv_sem, group_at, seq_at, dst=None):
    pltpu.make_async_remote_copy(
        src_ref=ref,
        dst_ref=ref if dst is None else dst,
        send_sem=send_sem,
        recv_sem=recv_sem,
        device_id={"group": group_at, "seq": seq_at},
        device_id_type=MESH,
    ).start()


def wait(ref, sem):
    pltpu.make_async_copy(ref, ref, sem).wait()


def line_kernel(
    n, tokens, gain, w_key, w_value, lengths, pages, freq, out,
    wide_gain, wbuf, xbuf, pbuf, rbuf, raw, found, page_of, found_sem, cosine, sine,
    load_sem, tok_sem, ys, yr, fr, fq, zi, zo, zr, xs, xo, xr, xq, cs, cr, hs, hr, rs, rr,
):
    chunks, depth = wbuf.shape[0], wbuf.shape[1]
    half, width = wbuf.shape[5], wbuf.shape[6]
    per_kind = chunks // 2
    group = lax.axis_index("group")
    me = lax.axis_index("seq")
    core, y, z = lax.rem(me, 2), lax.rem(me // 2, 2), me // 4
    other_core, other_y, other_group = 1 - core, 1 - y, 1 - group
    high = z // (depth // 2)
    is_end = (z == 0) | (z == depth - 1)

    def at(p):
        return p + high * (depth - 1 - 2 * p)

    def seq_of(z_at, y_at, core_at):
        return (z_at * 2 + y_at) * 2 + core_at

    to_y = seq_of(z, other_y, core)
    to_core = seq_of(z, y, other_core)

    def piece(j, zz, yy, part):
        return wbuf.at[j, zz, yy, core, part]

    def line(j, zz, yy):
        return wbuf.at[j, zz, yy, core]

    def pair(j, zz, part):
        return wbuf.at[j, zz, :, core, part]

    def layer(j, zz):
        return wbuf.at[j, zz, :, core]

    def load(j):
        w_ref = w_key if j < per_kind else w_value
        columns = pl.ds((j % per_kind) * width, width)
        return [
            pltpu.make_async_copy(
                w_ref.at[pl.ds(part * half, half), columns], piece(j, z, y, part), load_sem.at[j, part]
            )
            for part in range(2)
        ]

    for j in range(chunks):
        for copy in load(j):
            copy.start()
    token_copy = pltpu.make_async_copy(tokens, xbuf, tok_sem)
    token_copy.start()

    barrier = pltpu.get_barrier_semaphore()

    def greet(group_at, seq_at):
        pl.semaphore_signal(
            barrier, inc=1, device_id={"group": group_at, "seq": seq_at}, device_id_type=MESH
        )

    greet(other_group, me)
    for step in range(1, n):
        greet(group, lax.rem(me + step, n))
    pl.semaphore_wait(barrier, n)

    def over_y(ref, j, sem):
        copy_to(ref, ys.at[j], sem, group, to_y)

    def over_x(ref, j, sem):
        copy_to(ref, xs.at[j], sem, other_group, me)

    def inward(ref, j, zz, p):
        copy_to(ref, zi.at[j], zr.at[j, zz], group, seq_of(at(p), y, core))

    def outward(ref, j, zz):
        copy_to(ref, zo.at[j], zr.at[j, zz], group, seq_of(at(0), y, core))

    def to_partner(j, zz):
        copy_to(layer(j, zz), cs.at[j], cr.at[j], group, to_core)

    def loaded(j):
        for copy in load(j):
            copy.wait()

    def end_waits(j, what, k):
        form, both = CHUNKS[j]
        zz = at(k)
        if what == CROSS:
            return [(line(j, z, other_y) if both else piece(j, z, other_y, group), yr.at[j])]
        if what == ACROSS:
            return [(piece(j, z, other_y, other_group), xo.at[j])]
        if what == ALONG:
            return [(pair(j, zz, group) if form == PAIRED else piece(j, zz, y, group), zr.at[j, zz])]
        from_x = (piece(j, zz, y, other_group), xr.at[j, zz])
        from_y = (piece(j, zz, other_y, group), fr.at[j, zz])
        if what == FACE:
            return [(pair(j, zz, other_group), xr.at[j, zz])] if form == PAIRED else [from_x]
        if what == SIDE:
            return [from_y]
        if form == SPLIT:
            return [from_y, (piece(j, zz, other_y, other_group), fq.at[j, zz])]
        return [from_x, (piece(j, zz, other_y, other_group), xq.at[j, zz])]

    def end_sends(j, what, k):
        form, both = CHUNKS[j]
        zz = at(k)
        partner = functools.partial(to_partner, j, zz)
        if what == BEGIN:
            mine = line(j, z, y) if both else piece(j, z, y, group)
            return [lambda: over_y(mine, j, yr.at[j]), lambda: inward(line(j, z, y), j, z, 1)]
        if what == CROSS:
            if both:
                return [lambda: inward(line(j, z, other_y), j, z, 1), lambda: to_partner(j, z)]
            return [
                lambda: inward(piece(j, z, other_y, group), j, z, 1),
                lambda: over_x(piece(j, z, other_y, group), j, xo.at[j]),
            ]
        if what == ACROSS:
            return [lambda: inward(piece(j, z, other_y, other_group), j, z, 1), lambda: to_partner(j, z)]
        if what == ALONG:
            one = piece(j, zz, y, group)
            by_x = lambda: over_x(one, j, xr.at[j, zz])
            by_y = lambda: over_y(one, j, fr.at[j, zz])
            if form == PAIRED:
                return [lambda: over_x(pair(j, zz, group), j, xr.at[j, zz])]
            return [by_x, by_y] if form == SPLIT else [by_y, by_x]
        if what == FACE and form == SPLIT:
            return [lambda: over_y(piece(j, zz, y, other_group), j, fq.at[j, zz])]
        if what == SIDE:
            return [lambda: over_x(piece(j, zz, other_y, group), j, xq.at[j, zz])]
        return [partner]

    def inner_waits(j, what, p):
        zz = at(p)
        if what == CROSS:
            return [(piece(j, z, other_y, group), yr.at[j])]
        if what == ACROSS:
            return [(piece(j, z, other_y, other_group), xo.at[j])]
        if what == ALONG:
            return [(layer(j, zz) if p == 0 else pair(j, zz, group), zr.at[j, zz])]
        return [(pair(j, zz, other_group), xr.at[j, zz])]

    def inner_sends(j, what, p):
        form, _ = CHUNKS[j]
        zz = at(p)
        if what == BEGIN:
            mine = piece(j, z, y, group)
            return [
                lambda: over_y(mine, j, yr.at[j]),
                lambda: outward(mine, j, z),
                lambda: inward(mine, j, z, 2),
            ]
        if what == CROSS:
            crossed = piece(j, z, other_y, group)
            out_too = [lambda: outward(crossed, j, z)] if form == PAIRED else []
            return [lambda: inward(crossed, j, z, 2)] + out_too + [lambda: over_x(crossed, j, xo.at[j])]
        if what == ACROSS:
            return [lambda: to_partner(j, z)]
        if what == ALONG and p == 0:
            return [lambda: inward(pair(j, zz, group), j, zz, 2), lambda: to_partner(j, zz)]
        if what == ALONG:
            kept = pair(j, zz, group) if form == PAIRED else piece(j, zz, y, group)
            return [lambda: outward(kept, j, zz), lambda: over_x(pair(j, zz, group), j, xr.at[j, zz])]
        return [lambda: to_partner(j, zz)]

    first_chunk = [sum(GROUPS[:g]) for g in range(len(GROUPS))]

    def spot(g, region):
        j, wide = first_chunk[g], GROUPS[g] * width
        rows = pl.ds(region * BLOCK, BLOCK)
        return (
            pbuf.at[g, rows, pl.ds(0, wide)],
            out.at[j // per_kind, rows, pl.ds((j % per_kind) * width, wide)],
        )

    def page_to(g, region):
        src, dst = spot(g, region)
        there = lax.rem(me + region - REACH + n, n)
        z_there, y_there = there // 4, lax.rem(there // 2, 2)

        def direct():
            copy_to(src, hs.at[g, region], hr.at[g, region], group, there, dst)

        if g not in RELAYED:
            direct()
            return
        slot = 0 if abs(region - REACH) == 2 else 1
        around = ((z_there == 0) | (z_there == depth - 1)) & (z_there != z)
        z_by = 1 + (z_there // (depth - 1)) * (depth - 3)
        by = seq_of(z_by, y_there, lax.rem(there, 2))

        @pl.when(around)
        def _():
            held = rbuf.at[RELAYED.index(g), slot, :, pl.ds(0, GROUPS[g] * width)]
            copy_to(src, hs.at[g, region], rr.at[g, slot], group, by, held)

        @pl.when(jnp.logical_not(around))
        def _():
            direct()

    def pages_on_chip(g):
        src, dst = spot(g, REACH)
        pltpu.make_async_copy(src, dst, hr.at[g, REACH]).start()
        for region, on in ((3, core == 0), (1, core == 1)):
            @pl.when(on)
            def _():
                src, dst = spot(g, region)
                copy_to(src, hs.at[g, region], hr.at[g, region], group, to_core, dst)

    def pages_off_chip(g, way, which):
        if which == 0:
            page_to(g, 4 if way == UP else 0)
            return

        @pl.when(core == (1 if way == UP else 0))
        def _():
            page_to(g, 3 if way == UP else 1)

    def pass_pages(g):
        def one(slot, region):
            held = rbuf.at[RELAYED.index(g), slot, :, pl.ds(0, GROUPS[g] * width)]
            wait(held, rr.at[g, slot])
            _, dst = spot(g, region)
            copy_to(held, rs.at[g, slot], hr.at[g, region], group, seq_of(at(0), y, core), dst)

        for side, regions in ((0, (4, 3)), (1, (0, 1))):
            @pl.when(y == side)
            def _():
                one(0, regions[0])

                @pl.when(core == side)
                def _():
                    one(1, regions[1])

    def run(steps, waits, sends, seen):
        for what, j, k, which in steps:
            if what in (UP, DOWN):
                pages_off_chip(j, what, which)
            elif what == RELAY:
                pass_pages(j)
            elif what == BEGIN:
                if j not in seen:
                    seen.add(j)
                    loaded(j)
                sends(j, what, k)[which]()
            elif which < 0:
                for ref, sem in waits(j, what, k):
                    wait(ref, sem)
            else:
                sends(j, what, k)[which]()

    work = Work(n, (gain, lengths, pages, freq, wide_gain, xbuf, raw, found, page_of, found_sem, cosine, sine), me)
    tok_rows = work.tok_rows

    def project(g):
        at_chunk, wide = first_chunk[g], GROUPS[g] * width
        blocks = []
        for j in range(at_chunk, at_chunk + GROUPS[g]):
            wait(wbuf.at[j, :, :, other_core], cr.at[j])
            blocks.append(wbuf[j].reshape(work.features, width))
        weights = blocks[0] if len(blocks) == 1 else jnp.concatenate(blocks, axis=1)

        def put(at_row, page):
            pbuf[g, at_row : at_row + PAGE, 0:wide] = page

        work.project(weights, at_chunk < per_kind, put)
        pages_on_chip(g)

    sixteenth = tok_rows // 16
    jobs = [lambda: (work.spread_gain(), token_copy.wait())]
    jobs += [functools.partial(work.normalise, i * sixteenth, sixteenth) for i in range(16)]
    jobs += [work.find_pages]
    jobs += [functools.partial(work.angles, i * (tok_rows // 2), tok_rows // 2) for i in range(2)]
    jobs, projects = iter(jobs), iter(range(len(GROUPS)))
    inner, second = jnp.logical_not(is_end), y != high
    first = jnp.logical_not(second)
    kinds = (
        (is_end & first, END_FIRST, end_waits, end_sends, set()),
        (is_end & second, END_SECOND, end_waits, end_sends, set()),
        (inner & first, INNER_FIRST, inner_waits, inner_sends, set()),
        (inner & second, INNER_SECOND, inner_waits, inner_sends, set()),
    )
    for stretch in range(len(COMPUTE) + 1):
        if stretch:
            if COMPUTE[stretch - 1]:
                project(next(projects))
            else:
                next(jobs)()
        for here, steps, waits, sends, seen in kinds:
            if steps[stretch]:

                @pl.when(here)
                def _():
                    run(steps[stretch], waits, sends, seen)

    def count(pieces, sem):
        wait(xbuf.at[pl.ds(0, half), pl.ds(0, pieces * width)], sem)

    for j in range(chunks):
        form, both = CHUNKS[j]
        wait(wbuf.at[j, :, :, core], cs.at[j])

        @pl.when(is_end)
        def _():
            far = depth - 1
            count((2 if both else 1) + far * {PAIRED: 0, SPLIT: 2, TURNED: 1}[form], ys.at[j])
            count(far * {PAIRED: 2, SPLIT: 1, TURNED: 2}[form] + (0 if both else 1), xs.at[j])
            count(4, zi.at[j])

        @pl.when(jnp.logical_not(is_end))
        def _():
            count(1, ys.at[j])
            count(2 * depth - 3, xs.at[j])
            count(4, zi.at[j])
            count((depth - 1) * (2 if form == PAIRED else 1), zo.at[j])

    for g in range(len(GROUPS)):
        for region in range(REGIONS):
            src, dst = spot(g, region)
            wait(dst, hr.at[g, region])
            if region != REACH:
                wait(src, hs.at[g, region])
        if g in RELAYED:
            held = rbuf.at[RELAYED.index(g), 0, :, pl.ds(0, GROUPS[g] * width)]

            @pl.when(jnp.logical_not(is_end))
            def _():
                wait(held, rs.at[g, 0])

                @pl.when(core == y)
                def _():
                    wait(held, rs.at[g, 1])


def loop_kernel(
    n, tokens, gain, w_key, w_value, lengths, pages, freq, out,
    wide_gain, wbuf, xbuf, pbuf, raw, found, page_of, found_sem, cosine, sine,
    load_sem, tok_sem, ys, yr, zs, zr, xs, xr, cs, cr, hs, hr,
):
    chunks, depth = wbuf.shape[0], wbuf.shape[1]
    half, width = wbuf.shape[5], wbuf.shape[6]
    per_kind = chunks // 2
    group = lax.axis_index("group")
    me = lax.axis_index("seq")
    core, y, z = lax.rem(me, 2), lax.rem(me // 2, 2), me // 4
    other_core, other_y, other_group = 1 - core, 1 - y, 1 - group

    def seq_of(z_at, y_at, core_at):
        return (z_at * 2 + y_at) * 2 + core_at

    def piece(j, z_at, y_at, part):
        return wbuf.at[j, z_at, y_at, core, part]

    loads = []
    for j in range(chunks):
        w_ref = w_key if j < per_kind else w_value
        columns = pl.ds((j % per_kind) * width, width)
        for part in range(2):
            copy = pltpu.make_async_copy(
                w_ref.at[pl.ds(part * half, half), columns], piece(j, z, y, part), load_sem.at[j, part]
            )
            copy.start()
            loads.append(copy)
    token_copy = pltpu.make_async_copy(tokens, xbuf, tok_sem)
    token_copy.start()

    to_y = seq_of(z, other_y, core)
    to_core = seq_of(z, y, other_core)
    has_up, has_down = z + 1 < depth, z > 0
    up = seq_of(lax.rem(z + 1, depth), y, core)
    down = seq_of(lax.rem(z + depth - 1, depth), y, core)

    barrier = pltpu.get_barrier_semaphore()

    def greet(group_at, seq_at):
        pl.semaphore_signal(
            barrier, inc=1, device_id={"group": group_at, "seq": seq_at}, device_id_type=MESH
        )

    for seq_at in (up, down, to_y, to_core):
        greet(group, seq_at)
    greet(other_group, me)
    for region in range(REGIONS):
        if region != REACH:
            greet(group, lax.rem(me + region - REACH + n, n))
    pl.semaphore_wait(barrier, 5 + REGIONS - 1)

    def to_partner(j, ref):
        copy_to(ref, cs.at[j], cr.at[j], group, to_core)

    def go(j, z_at, y_at, k, way):
        @pl.when(has_up if way == 0 else has_down)
        def _():
            copy_to(piece(j, z_at, y_at, group), zs.at[j, way, k], zr.at[j, y_at, z_at], group,
                    up if way == 0 else down)

    def begin(j):
        for part in (0, 1):
            loads[2 * j + part].wait()
        for part in (0, 1):
            copy_to(piece(j, z, y, part), ys.at[j], yr.at[j, part], group, to_y)
            to_partner(j, piece(j, z, y, part))
        go(j, z, y, 0, 0)
        go(j, z, y, 0, 1)

    def cross(j):
        for part in (0, 1):
            wait(piece(j, z, other_y, part), yr.at[j, part])
            to_partner(j, piece(j, z, other_y, part))
        go(j, z, other_y, 0, 0)
        go(j, z, other_y, 0, 1)

    def both(k, visit):
        @pl.when(z - k >= 0)
        def _():
            visit(z - k, 0)

        @pl.when(z + k < depth)
        def _():
            visit(z + k, 1)

    def along(j, k):
        def visit(zz, way):
            for y_at in (y, other_y):
                ref = piece(j, zz, y_at, group)
                wait(ref, zr.at[j, y_at, zz])
                go(j, zz, y_at, k, way)
                copy_to(ref, xs.at[j], xr.at[j, y_at, zz], other_group, me)
                to_partner(j, ref)

        both(k, visit)

    def finish(j, k):
        def visit(zz, way):
            for y_at in (y, other_y):
                ref = piece(j, zz, y_at, other_group)
                wait(ref, xr.at[j, y_at, zz])
                to_partner(j, ref)

        both(k, visit)

    work = Work(n, (gain, lengths, pages, freq, wide_gain, xbuf, raw, found, page_of, found_sem, cosine, sine), me)

    def project(j):
        wait(wbuf.at[j, :, :, other_core], cr.at[j])
        for at in range(0, width, TILE):
            def put(at_row, page):
                pbuf[j, at_row : at_row + PAGE, at : at + TILE] = page

            weights = wbuf[j, :, :, :, :, :, at : at + TILE].reshape(work.features, TILE)
            work.project(weights, j < per_kind, put)

    def spot(j, region):
        rows = pl.ds(region * BLOCK, BLOCK)
        return (
            pbuf.at[j, rows, :],
            out.at[j // per_kind, rows, pl.ds((j % per_kind) * width, width)],
        )

    def hand_over(j):
        for region in range(REGIONS):
            src, dst = spot(j, region)
            if region == REACH:
                pltpu.make_async_copy(src, dst, hr.at[j, region]).start()
            else:
                copy_to(src, hs.at[j, region], hr.at[j, region], group,
                        lax.rem(me + region - REACH + n, n), dst)

    for j in range(chunks):
        begin(j)
    work.spread_gain()
    token_copy.wait()
    work.normalise(0, work.tok_rows)
    work.find_pages()
    work.angles(0, work.tok_rows)
    for j in range(chunks):
        cross(j)
        lax.fori_loop(1, depth, lambda k, carry: (along(j, k), carry)[1], 0)
        lax.fori_loop(1, depth, lambda k, carry: (finish(j, k), carry)[1], 0)
        project(j)
        hand_over(j)

    for j in range(chunks):
        wait(wbuf.at[j, z, y, core], ys.at[j])
        wait(wbuf.at[j, 1:, :, core, group], xs.at[j])
        wait(wbuf.at[j, :, :, core], cs.at[j])
        sent = wbuf.at[j, 0, :, core, group]

        def drain(k, carry):
            @pl.when(has_up & (z - k >= 0))
            def _():
                wait(sent, zs.at[j, 0, k])

            @pl.when(has_down & (z + k < depth))
            def _():
                wait(sent, zs.at[j, 1, k])

            return carry

        lax.fori_loop(0, depth, drain, 0)
        for region in range(REGIONS):
            src, dst = spot(j, region)
            wait(dst, hr.at[j, region])
            if region != REACH:
                wait(src, hs.at[j, region])


def on_device(n, tokens, norm_gain, w_key, w_value, lengths, page_table):
    tok_rows, features = tokens.shape
    columns = w_key.shape[1]
    freq = ROPE_THETA ** (-(np.arange(HEAD // 2) * 2.0 / HEAD))
    freq = np.concatenate([freq, freq]).astype(np.float32)[None, :]
    depth = n // 4
    half = w_key.shape[0] // 2
    dma = pltpu.SemaphoreType.DMA
    vmem = pl.BlockSpec(memory_space=pltpu.VMEM)
    smem = pl.BlockSpec(memory_space=pltpu.SMEM)
    hbm = pl.BlockSpec(memory_space=pl.ANY)
    in_line = depth == LAYERS
    chunks = len(CHUNKS) if in_line else LOOP_CHUNKS
    groups = len(GROUPS) if in_line else chunks
    width = 2 * columns // chunks
    wide = width * max(GROUPS) if in_line else width
    scratch = [
        pltpu.VMEM((1, features), jnp.float32),
        pltpu.VMEM((chunks, depth, 2, 2, 2, half, width), jnp.bfloat16),
        pltpu.VMEM((tok_rows, features), jnp.bfloat16),
        pltpu.VMEM((groups, ROWS, wide), jnp.bfloat16),
    ]
    if in_line:
        scratch.append(pltpu.VMEM((max(len(RELAYED), 1), 2, BLOCK, wide), jnp.bfloat16))
    scratch += [
        pltpu.VMEM((tok_rows // PAGE + 1, PAGE, TILE), jnp.bfloat16),
        pltpu.VMEM((1, HEAD), jnp.int32),
        pltpu.SMEM((1, HEAD), jnp.int32),
        dma,
        pltpu.VMEM((tok_rows, HEAD), jnp.float32),
        pltpu.VMEM((tok_rows, HEAD), jnp.float32),
        dma((chunks, 2)),
        dma,
    ]
    each, by_layer, by_region = dma((chunks,)), dma((chunks, depth)), dma((groups, REGIONS))
    if in_line:
        slots = dma((groups, 2))
        scratch += [each, each, by_layer, by_layer, each, each, by_layer, each, each, by_layer, by_layer,
                    each, each, by_region, by_region, slots, slots]
    else:
        by_line = dma((chunks, 2, depth))
        scratch += [each, dma((chunks, 2)), by_line, by_line, each, by_line, each, each,
                    by_region, by_region]
    cache = pl.pallas_call(
        functools.partial(line_kernel if in_line else loop_kernel, n),
        out_shape=pltpu.VMEM((2, ROWS, columns), jnp.bfloat16),
        in_specs=[hbm, vmem, hbm, hbm, smem, smem, vmem],
        out_specs=vmem,
        scratch_shapes=scratch,
        compiler_params=pltpu.CompilerParams(
            collective_id=0, has_side_effects=True, vmem_limit_bytes=60 * 2**20
        ),
    )(tokens, norm_gain.reshape(-1, HEAD), w_key, w_value, lengths, page_table, freq)
    return cache.reshape(2, SLOTS, PAGE, columns)


def solution(mesh):
    placed = (
        P(("group", "seq"), None),
        P(),
        P("seq", None),
        P("seq", None),
        P("group"),
        P(("group", "seq")),
    )
    return jax.shard_map(
        functools.partial(on_device, mesh.shape["seq"]),
        mesh=mesh,
        in_specs=placed,
        out_specs=P(None, ("group", "seq"), None, None),
        check_vma=False,
    )
```

```python
import functools

import jax
import jax.numpy as jnp
import numpy as np
from jax import lax
from jax.experimental import pallas as pl
from jax.experimental.pallas import tpu as pltpu
from jax.sharding import PartitionSpec as P

HEAD = 128
PAGE = 16
REACH = 2
CAP = 8
SLOTS = 40
REGIONS = 2 * REACH + 1
BLOCK = CAP * PAGE
ROWS = SLOTS * PAGE

ROPE_THETA = 500000.0
EPS = 1e-05

TILE = 256
MESH = pl.DeviceIdType.MESH

PAIRED, SPLIT, TURNED = 0, 1, 2
CHUNKS = ((SPLIT, True), (PAIRED, False), (PAIRED, True), (SPLIT, True), (PAIRED, True), (SPLIT, True), (PAIRED, True), (PAIRED, True))
GROUPS = (1, 1, 1, 1, 1, 1, 1, 1)
RELAYED = (1, 5)

LAYERS = 4
LOOP_CHUNKS = 8

BEGIN, CROSS, ACROSS, ALONG, FACE, SIDE, SETTLE, UP, DOWN, RELAY = range(10)
COMPUTE = (0,0,0,0,0,0,0,0,0,0,0,0,0,0,0,0,0,0,0,0,1,1,1,1,1,1,1,1)
END_FIRST = (
    ((BEGIN, 0, 0, 0), (BEGIN, 0, 0, 1),),
    (),
    (),
    ((BEGIN, 1, 0, 0),),
    (),
    (),
    ((BEGIN, 1, 0, 1),),
    (),
    (),
    (),
    (),
    (),
    (),
    (),
    ((BEGIN, 2, 0, 0),),
    (),
    (),
    ((ALONG, 0, 1, -1), (ALONG, 0, 1, 0), (ALONG, 0, 1, 1),),
    (),
    ((CROSS, 0, 0, -1), (CROSS, 0, 0, 0), (CROSS, 0, 0, 1),),
    ((CROSS, 1, 0, -1), (CROSS, 1, 0, 0), (CROSS, 1, 0, 1), (FACE, 0, 1, -1), (FACE, 0, 1, 0), (BEGIN, 3, 0, 0),
     (ALONG, 3, 1, -1), (ALONG, 3, 1, 0), (ACROSS, 1, 0, -1), (ACROSS, 1, 0, 0), (ACROSS, 1, 0, 1),
     (ALONG, 1, 1, -1), (ALONG, 1, 1, 0), (BEGIN, 2, 0, 1), (CROSS, 2, 0, -1), (CROSS, 2, 0, 1),
     (SETTLE, 0, 1, -1), (SETTLE, 0, 1, 0), (ALONG, 2, 1, -1), (ALONG, 2, 1, 0), (ALONG, 3, 1, 1),
     (ALONG, 0, 2, -1), (ALONG, 0, 2, 1), (CROSS, 2, 0, 0), (FACE, 1, 1, -1), (FACE, 1, 1, 0), (FACE, 3, 1, -1),
     (FACE, 3, 1, 0), (ALONG, 0, 2, 0), (ALONG, 1, 2, -1), (ALONG, 1, 2, 0), (CROSS, 3, 0, -1),
     (CROSS, 3, 0, 1), (BEGIN, 4, 0, 0), (BEGIN, 3, 0, 1), (ALONG, 2, 2, -1), (FACE, 2, 1, -1),
     (FACE, 2, 1, 0), (SETTLE, 3, 1, -1), (SETTLE, 3, 1, 0), (ALONG, 2, 2, 0), (ALONG, 3, 2, -1),
     (FACE, 0, 2, -1), (FACE, 0, 2, 0), (CROSS, 3, 0, 0), (ALONG, 0, 3, -1), (ALONG, 3, 2, 1), (ALONG, 0, 3, 1),
     (FACE, 1, 2, -1), (FACE, 1, 2, 0), (ALONG, 0, 3, 0), (CROSS, 4, 0, -1), (CROSS, 4, 0, 1), (BEGIN, 4, 0, 1),
     (BEGIN, 5, 0, 0), (ALONG, 3, 2, 0), (CROSS, 4, 0, 0), (FACE, 2, 2, -1), (FACE, 2, 2, 0), (SETTLE, 0, 2, -1),
     (SETTLE, 0, 2, 0), (FACE, 0, 3, -1), (FACE, 0, 3, 0), (BEGIN, 5, 0, 1), (ALONG, 1, 3, -1),
     (ALONG, 1, 3, 0), (FACE, 3, 2, -1), (FACE, 3, 2, 0), (ALONG, 4, 1, -1), (ALONG, 4, 1, 0), (BEGIN, 6, 0, 0),
     (CROSS, 5, 0, -1), (CROSS, 5, 0, 1), (ALONG, 4, 2, -1), (ALONG, 4, 2, 0), (CROSS, 5, 0, 0),
     (BEGIN, 7, 0, 0), (SETTLE, 0, 3, -1), (SETTLE, 0, 3, 0), (FACE, 1, 3, -1), (FACE, 1, 3, 0),
     (BEGIN, 6, 0, 1), (ALONG, 2, 3, -1), (ALONG, 2, 3, 0), (ALONG, 5, 2, -1),),
    (),
    ((SETTLE, 3, 2, -1), (SETTLE, 3, 2, 0), (ALONG, 5, 1, -1), (ALONG, 5, 1, 1), (FACE, 4, 1, -1),
     (FACE, 4, 1, 0), (ALONG, 5, 2, 1), (ALONG, 3, 3, -1), (ALONG, 3, 3, 1), (ALONG, 3, 3, 0), (ALONG, 5, 1, 0),
     (CROSS, 6, 0, -1), (CROSS, 6, 0, 1), (CROSS, 6, 0, 0), (FACE, 4, 2, -1), (FACE, 4, 2, 0), (CROSS, 7, 0, -1),
     (CROSS, 7, 0, 1), (ALONG, 5, 2, 0), (BEGIN, 7, 0, 1), (FACE, 2, 3, -1), (FACE, 2, 3, 0), (ALONG, 6, 1, -1),
     (ALONG, 6, 1, 0), (DOWN, 0, 0, 0), (FACE, 3, 3, -1), (FACE, 3, 3, 0), (UP, 0, 0, 0),),
    ((ALONG, 4, 3, -1), (UP, 0, 0, 1), (CROSS, 7, 0, 0), (ALONG, 4, 3, 0), (FACE, 5, 1, -1), (FACE, 5, 1, 0),
     (FACE, 5, 2, -1), (FACE, 5, 2, 0), (SETTLE, 5, 1, -1), (SETTLE, 5, 1, 0), (DOWN, 0, 0, 1),
     (SETTLE, 3, 3, -1), (SETTLE, 3, 3, 0), (ALONG, 6, 2, -1), (UP, 1, 0, 0), (FACE, 6, 1, -1),
     (FACE, 6, 1, 0), (ALONG, 5, 3, -1), (ALONG, 5, 3, 0), (ALONG, 5, 3, 1), (ALONG, 6, 2, 0), (DOWN, 2, 0, 0),
     (UP, 2, 0, 0), (FACE, 5, 3, -1), (FACE, 5, 3, 0), (FACE, 4, 3, -1), (FACE, 4, 3, 0), (DOWN, 1, 0, 1),
     (SETTLE, 5, 2, -1), (SETTLE, 5, 2, 0), (ALONG, 7, 1, -1), (ALONG, 7, 1, 0), (UP, 1, 0, 1),
     (DOWN, 2, 0, 1), (UP, 2, 0, 1),),
    ((UP, 3, 0, 0), (DOWN, 1, 0, 0),),
    ((DOWN, 3, 0, 1), (UP, 3, 0, 1), (UP, 4, 0, 0), (FACE, 6, 2, -1), (FACE, 6, 2, 0), (ALONG, 6, 3, -1),
     (ALONG, 6, 3, 0), (DOWN, 3, 0, 0), (ALONG, 7, 2, -1), (ALONG, 7, 2, 0), (DOWN, 4, 0, 0), (SETTLE, 5, 3, -1),
     (SETTLE, 5, 3, 0), (DOWN, 4, 0, 1), (UP, 4, 0, 1), (FACE, 7, 1, -1), (FACE, 7, 1, 0),),
    ((UP, 5, 0, 0), (DOWN, 5, 0, 0), (ALONG, 7, 3, -1), (ALONG, 7, 3, 0), (UP, 5, 0, 1), (DOWN, 5, 0, 1),
     (FACE, 6, 3, -1), (FACE, 6, 3, 0), (FACE, 7, 2, -1), (FACE, 7, 2, 0),),
    ((DOWN, 6, 0, 0), (UP, 6, 0, 0), (UP, 6, 0, 1), (DOWN, 6, 0, 1), (FACE, 7, 3, -1), (FACE, 7, 3, 0),
     ),
    ((DOWN, 7, 0, 0), (DOWN, 7, 0, 1), (UP, 7, 0, 0), (UP, 7, 0, 1),),
)
END_SECOND = (
    ((BEGIN, 0, 0, 0), (BEGIN, 0, 0, 1),),
    (),
    (),
    (),
    ((BEGIN, 1, 0, 0),),
    ((BEGIN, 1, 0, 1),),
    (),
    (),
    (),
    (),
    (),
    (),
    (),
    (),
    (),
    ((BEGIN, 2, 0, 0),),
    (),
    (),
    ((ALONG, 0, 1, -1), (ALONG, 0, 1, 0), (ALONG, 0, 1, 1),),
    (),
    ((CROSS, 0, 0, -1), (CROSS, 0, 0, 0), (CROSS, 0, 0, 1), (CROSS, 1, 0, -1), (CROSS, 1, 0, 0),
     (CROSS, 1, 0, 1), (ALONG, 3, 1, -1), (ALONG, 3, 1, 0), (FACE, 0, 1, -1), (FACE, 0, 1, 0), (BEGIN, 3, 0, 0),
     (ACROSS, 1, 0, -1), (ACROSS, 1, 0, 0), (ACROSS, 1, 0, 1), (ALONG, 1, 1, -1), (ALONG, 1, 1, 0),
     (FACE, 3, 1, -1), (FACE, 3, 1, 0), (BEGIN, 2, 0, 1), (CROSS, 2, 0, -1), (CROSS, 2, 0, 1), (ALONG, 2, 1, -1),
     (ALONG, 2, 1, 0), (ALONG, 3, 1, 1), (SETTLE, 0, 1, -1), (SETTLE, 0, 1, 0), (CROSS, 2, 0, 0),
     (FACE, 1, 1, -1), (FACE, 1, 1, 0), (ALONG, 0, 2, -1), (ALONG, 0, 2, 1), (ALONG, 0, 2, 0), (BEGIN, 4, 0, 0),
     (CROSS, 3, 0, -1), (CROSS, 3, 0, 1), (CROSS, 3, 0, 0), (BEGIN, 3, 0, 1), (ALONG, 1, 2, -1),
     (ALONG, 1, 2, 0), (FACE, 2, 1, -1), (FACE, 2, 1, 0), (ALONG, 2, 2, -1), (ALONG, 2, 2, 0), (SETTLE, 3, 1, -1),
     (SETTLE, 3, 1, 0), (FACE, 0, 2, -1), (FACE, 0, 2, 0), (ALONG, 3, 2, -1), (ALONG, 0, 3, -1),
     (ALONG, 0, 3, 0), (ALONG, 0, 3, 1), (FACE, 1, 2, -1), (FACE, 1, 2, 0), (ALONG, 3, 2, 1), (BEGIN, 4, 0, 1),
     (ALONG, 3, 2, 0), (ALONG, 4, 1, -1), (ALONG, 4, 1, 0), (BEGIN, 5, 0, 0), (CROSS, 4, 0, -1),
     (CROSS, 4, 0, 0), (CROSS, 4, 0, 1), (SETTLE, 0, 2, -1), (SETTLE, 0, 2, 0), (FACE, 2, 2, -1),
     (FACE, 2, 2, 0), (ALONG, 1, 3, -1), (ALONG, 1, 3, 0), (BEGIN, 5, 0, 1), (FACE, 0, 3, -1), (FACE, 0, 3, 0),
     (FACE, 3, 2, -1), (FACE, 3, 2, 0), (BEGIN, 6, 0, 0), (CROSS, 5, 0, -1), (CROSS, 5, 0, 0), (CROSS, 5, 0, 1),
     (ALONG, 4, 2, -1), (ALONG, 4, 2, 0), (SETTLE, 0, 3, -1), (SETTLE, 0, 3, 0), (FACE, 1, 3, -1),
     (FACE, 1, 3, 0), (FACE, 4, 1, -1), (FACE, 4, 1, 0), (SETTLE, 3, 2, -1), (SETTLE, 3, 2, 0),
     (BEGIN, 7, 0, 0), (ALONG, 2, 3, -1), (ALONG, 2, 3, 0), (ALONG, 5, 2, -1), (ALONG, 5, 2, 1),
     (BEGIN, 6, 0, 1),),
    (),
    ((ALONG, 5, 1, -1), (ALONG, 5, 1, 1), (ALONG, 5, 2, 0), (ALONG, 3, 3, -1), (ALONG, 3, 3, 0),
     (ALONG, 3, 3, 1), (ALONG, 5, 1, 0), (CROSS, 6, 0, -1), (CROSS, 6, 0, 0), (CROSS, 6, 0, 1),
     (FACE, 4, 2, -1), (FACE, 4, 2, 0), (BEGIN, 7, 0, 1), (FACE, 2, 3, -1), (FACE, 2, 3, 0), (CROSS, 7, 0, -1),
     (CROSS, 7, 0, 1), (ALONG, 6, 1, -1), (ALONG, 6, 1, 0), (DOWN, 0, 0, 0), (UP, 0, 0, 0), (UP, 1, 0, 1),
     (CROSS, 7, 0, 0), (FACE, 3, 3, -1), (FACE, 3, 3, 0), (ALONG, 4, 3, -1), (ALONG, 4, 3, 0), (FACE, 5, 1, -1),
     (FACE, 5, 1, 0), (FACE, 5, 2, -1), (FACE, 5, 2, 0), (SETTLE, 3, 3, -1), (SETTLE, 3, 3, 0),
     (DOWN, 0, 0, 1), (UP, 0, 0, 1),),
    ((DOWN, 1, 0, 0), (UP, 1, 0, 0), (ALONG, 5, 3, -1), (ALONG, 5, 3, 0), (ALONG, 5, 3, 1), (FACE, 6, 1, -1),
     (FACE, 6, 1, 0), (ALONG, 6, 2, -1), (ALONG, 6, 2, 0), (DOWN, 1, 0, 1), (SETTLE, 5, 1, -1),
     (SETTLE, 5, 1, 0), (DOWN, 2, 0, 0), (UP, 2, 0, 0),),
    ((FACE, 4, 3, -1), (FACE, 4, 3, 0), (SETTLE, 5, 2, -1), (SETTLE, 5, 2, 0), (DOWN, 2, 0, 1),
     (FACE, 5, 3, -1), (FACE, 5, 3, 0), (ALONG, 7, 1, -1), (ALONG, 7, 1, 0), (UP, 3, 0, 0), (UP, 2, 0, 1),
     ),
    ((DOWN, 3, 0, 1), (UP, 3, 0, 1), (FACE, 6, 2, -1), (FACE, 6, 2, 0), (ALONG, 6, 3, -1), (ALONG, 6, 3, 0),
     (UP, 4, 0, 0), (DOWN, 3, 0, 0), (DOWN, 4, 0, 0), (SETTLE, 5, 3, -1), (SETTLE, 5, 3, 0), (UP, 4, 0, 1),
     (DOWN, 4, 0, 1), (FACE, 7, 1, -1), (FACE, 7, 1, 0),),
    ((DOWN, 5, 0, 0), (UP, 5, 0, 0), (UP, 5, 0, 1), (DOWN, 5, 0, 1), (ALONG, 7, 2, -1), (ALONG, 7, 2, 0),
     (FACE, 6, 3, -1), (FACE, 6, 3, 0),),
    ((UP, 6, 0, 0), (DOWN, 6, 0, 0), (ALONG, 7, 3, -1), (ALONG, 7, 3, 0), (UP, 6, 0, 1), (DOWN, 6, 0, 1),
     (FACE, 7, 2, -1), (FACE, 7, 2, 0), (FACE, 7, 3, -1), (FACE, 7, 3, 0),),
    ((DOWN, 7, 0, 0), (UP, 7, 0, 0), (DOWN, 7, 0, 1), (UP, 7, 0, 1),),
)
INNER_FIRST = (
    ((BEGIN, 0, 0, 0), (BEGIN, 0, 0, 1), (BEGIN, 0, 0, 2), (BEGIN, 1, 0, 0),),
    (),
    ((BEGIN, 1, 0, 2), (BEGIN, 1, 0, 1),),
    ((BEGIN, 2, 0, 0),),
    (),
    (),
    ((BEGIN, 2, 0, 2),),
    ((BEGIN, 2, 0, 1),),
    ((BEGIN, 3, 0, 1),),
    (),
    ((BEGIN, 3, 0, 0),),
    (),
    (),
    ((CROSS, 0, 0, -1), (CROSS, 0, 0, 0), (CROSS, 0, 0, 1),),
    (),
    ((BEGIN, 4, 0, 0),),
    (),
    ((CROSS, 1, 0, -1), (CROSS, 1, 0, 0), (CROSS, 1, 0, 1), (CROSS, 1, 0, 2),),
    (),
    ((BEGIN, 5, 0, 0),),
    ((CROSS, 2, 0, -1), (CROSS, 2, 0, 0), (CROSS, 2, 0, 2), (CROSS, 2, 0, 1), (ACROSS, 0, 0, -1),
     (ACROSS, 0, 0, 0), (CROSS, 3, 0, -1), (CROSS, 3, 0, 0), (CROSS, 3, 0, 1), (BEGIN, 6, 0, 0),
     (BEGIN, 3, 0, 2), (ALONG, 0, 2, -1), (ALONG, 0, 2, 0), (ALONG, 0, 2, 1), (BEGIN, 7, 0, 0),
     (ACROSS, 1, 0, -1), (ACROSS, 1, 0, 0), (CROSS, 4, 0, -1), (ALONG, 1, 2, -1), (ALONG, 1, 2, 0),
     (ALONG, 1, 2, 1), (ACROSS, 2, 0, -1), (ACROSS, 2, 0, 0), (ALONG, 0, 0, -1), (ALONG, 0, 0, 0),
     (ALONG, 0, 0, 1), (ALONG, 2, 2, -1), (ALONG, 2, 2, 0), (CROSS, 5, 0, -1), (ALONG, 2, 2, 1),
     (CROSS, 6, 0, -1), (ACROSS, 3, 0, -1), (ACROSS, 3, 0, 0), (ALONG, 3, 2, -1), (ALONG, 1, 0, -1),
     (ALONG, 1, 0, 0), (ALONG, 1, 0, 1), (CROSS, 4, 0, 0), (FACE, 0, 2, -1), (FACE, 0, 2, 0), (CROSS, 7, 0, -1),
     (ALONG, 3, 2, 0), (ALONG, 0, 3, -1), (ALONG, 0, 3, 0), (BEGIN, 4, 0, 2), (ALONG, 0, 3, 1),
     (BEGIN, 4, 0, 1), (FACE, 1, 2, -1), (FACE, 1, 2, 0), (ALONG, 2, 0, -1), (ALONG, 2, 0, 0), (ALONG, 2, 0, 1),
     (CROSS, 4, 0, 1), (FACE, 2, 2, -1), (FACE, 2, 2, 0), (ALONG, 1, 3, -1), (ALONG, 1, 3, 0), (ALONG, 1, 3, 1),
     (ALONG, 3, 2, 1), (CROSS, 5, 0, 0), (CROSS, 4, 0, 2), (BEGIN, 5, 0, 2), (FACE, 0, 3, -1), (FACE, 0, 3, 0),
     (ALONG, 4, 2, -1), (ALONG, 4, 2, 0), (FACE, 1, 3, -1), (FACE, 1, 3, 0), (BEGIN, 6, 0, 2), (ALONG, 3, 0, -1),
     (ALONG, 3, 0, 0), (ALONG, 3, 0, 1), (ALONG, 2, 3, -1), (ALONG, 2, 3, 0), (ALONG, 2, 3, 1),
     (CROSS, 6, 0, 0), (ALONG, 4, 2, 1), (BEGIN, 5, 0, 1),),
    ((FACE, 3, 2, -1), (FACE, 3, 2, 0), (ALONG, 5, 2, -1), (ALONG, 5, 2, 0),),
    ((UP, 1, 0, 1), (BEGIN, 6, 0, 1), (ALONG, 4, 0, -1), (ALONG, 4, 0, 0), (ALONG, 4, 0, 1), (ACROSS, 4, 0, -1),
     (ACROSS, 4, 0, 0), (ALONG, 3, 3, -1), (ALONG, 3, 3, 0), (ALONG, 3, 3, 1), (UP, 1, 0, 0), (FACE, 2, 3, -1),
     (FACE, 2, 3, 0), (ALONG, 6, 2, -1), (CROSS, 7, 0, 0), (BEGIN, 7, 0, 2), (DOWN, 1, 0, 0), (CROSS, 6, 0, 1),
     (CROSS, 5, 0, 1),),
    ((DOWN, 1, 0, 1), (ALONG, 5, 0, -1), (ALONG, 5, 0, 0), (ALONG, 5, 0, 1), (FACE, 4, 2, -1), (FACE, 4, 2, 0),
     (ALONG, 6, 2, 0), (ALONG, 4, 3, -1), (ALONG, 4, 3, 0), (ALONG, 4, 3, 1), (FACE, 3, 3, -1),
     (FACE, 3, 3, 0), (ALONG, 5, 2, 1), (ALONG, 7, 2, -1),),
    ((ACROSS, 5, 0, -1), (ACROSS, 5, 0, 0), (UP, 0, 0, 0), (DOWN, 0, 0, 0), (ALONG, 6, 0, -1), (ALONG, 6, 0, 0),
     (ALONG, 6, 0, 1), (FACE, 4, 3, -1), (FACE, 4, 3, 0), (CROSS, 7, 0, 1), (ALONG, 5, 3, -1), (ALONG, 5, 3, 0),
     (ALONG, 5, 3, 1), (CROSS, 6, 0, 2), (BEGIN, 7, 0, 1), (UP, 0, 0, 1), (DOWN, 0, 0, 1), (ALONG, 6, 2, 1),
     (ALONG, 7, 2, 0), (FACE, 5, 2, -1), (FACE, 5, 2, 0), (ALONG, 6, 3, -1), (ALONG, 6, 3, 0), (ALONG, 7, 0, -1),
     (ALONG, 7, 0, 0), (ALONG, 7, 0, 1), (UP, 2, 0, 0), (FACE, 5, 3, -1), (FACE, 5, 3, 0), (DOWN, 2, 0, 0),
     (CROSS, 7, 0, 2), (ALONG, 6, 3, 1), (ACROSS, 6, 0, -1), (ACROSS, 6, 0, 0), (UP, 2, 0, 1), (DOWN, 2, 0, 1),
     (UP, 3, 0, 0), (ALONG, 7, 2, 1), (FACE, 6, 2, -1), (FACE, 6, 2, 0), (ALONG, 7, 3, -1), (ALONG, 7, 3, 0),
     (UP, 3, 0, 1), (DOWN, 3, 0, 1), (DOWN, 3, 0, 0), (FACE, 6, 3, -1), (FACE, 6, 3, 0), (ALONG, 7, 3, 1),
     ),
    ((UP, 4, 0, 0),),
    ((DOWN, 5, 0, 0), (UP, 5, 0, 0), (UP, 5, 0, 1), (ACROSS, 7, 0, -1), (ACROSS, 7, 0, 0), (DOWN, 5, 0, 1),
     ),
    ((DOWN, 4, 0, 1), (UP, 4, 0, 1), (DOWN, 4, 0, 0), (FACE, 7, 3, -1), (FACE, 7, 3, 0), (FACE, 7, 2, -1),
     (FACE, 7, 2, 0), (RELAY, 1, 0, 0), (DOWN, 6, 0, 0),),
    ((UP, 6, 0, 1), (DOWN, 6, 0, 1), (UP, 6, 0, 0), (DOWN, 7, 0, 0), (UP, 7, 0, 0), (DOWN, 7, 0, 1),
     (RELAY, 5, 0, 0), (UP, 7, 0, 1),),
)
INNER_SECOND = (
    ((BEGIN, 0, 0, 0), (BEGIN, 0, 0, 1), (BEGIN, 0, 0, 2), (BEGIN, 1, 0, 0),),
    ((BEGIN, 1, 0, 1), (BEGIN, 1, 0, 2),),
    (),
    ((BEGIN, 2, 0, 0),),
    ((BEGIN, 2, 0, 2),),
    (),
    (),
    ((BEGIN, 2, 0, 1),),
    (),
    ((BEGIN, 3, 0, 1),),
    (),
    ((BEGIN, 3, 0, 0), (BEGIN, 4, 0, 0),),
    ((CROSS, 0, 0, -1), (CROSS, 0, 0, 0), (CROSS, 0, 0, 1),),
    (),
    (),
    (),
    ((CROSS, 1, 0, -1), (CROSS, 1, 0, 0), (CROSS, 1, 0, 1), (CROSS, 1, 0, 2),),
    (),
    (),
    ((BEGIN, 5, 0, 0),),
    ((CROSS, 2, 0, -1), (CROSS, 2, 0, 0), (CROSS, 2, 0, 2), (CROSS, 2, 0, 1), (BEGIN, 3, 0, 2),
     (CROSS, 3, 0, -1), (CROSS, 3, 0, 1), (ALONG, 0, 2, -1), (ALONG, 0, 2, 0), (ALONG, 0, 2, 1),
     (CROSS, 3, 0, 0), (ACROSS, 0, 0, -1), (ACROSS, 0, 0, 0), (BEGIN, 7, 0, 0), (CROSS, 4, 0, -1),
     (ALONG, 1, 2, -1), (ALONG, 1, 2, 0), (ALONG, 1, 2, 1), (ALONG, 2, 2, -1), (CROSS, 5, 0, -1),
     (ALONG, 0, 0, -1), (ALONG, 0, 0, 0), (ALONG, 0, 0, 1), (ALONG, 2, 2, 0), (ACROSS, 1, 0, -1),
     (ACROSS, 1, 0, 0), (ACROSS, 2, 0, -1), (ACROSS, 2, 0, 0), (BEGIN, 6, 0, 0), (CROSS, 6, 0, -1),
     (ALONG, 3, 2, -1), (ALONG, 2, 2, 1), (FACE, 0, 2, -1), (FACE, 0, 2, 0), (ALONG, 1, 0, -1),
     (ALONG, 1, 0, 0), (ALONG, 1, 0, 1), (CROSS, 7, 0, -1), (ACROSS, 3, 0, -1), (ACROSS, 3, 0, 0),
     (ALONG, 3, 2, 0), (BEGIN, 4, 0, 2), (ALONG, 0, 3, -1), (ALONG, 0, 3, 0), (BEGIN, 4, 0, 1),
     (ALONG, 0, 3, 1), (CROSS, 4, 0, 0), (FACE, 1, 2, -1), (FACE, 1, 2, 0), (ALONG, 2, 0, -1), (ALONG, 2, 0, 0),
     (ALONG, 2, 0, 1), (CROSS, 4, 0, 1), (ALONG, 1, 3, -1), (ALONG, 1, 3, 0), (FACE, 2, 2, -1),
     (FACE, 2, 2, 0), (ALONG, 1, 3, 1), (ALONG, 3, 2, 1), (BEGIN, 5, 0, 2), (ALONG, 4, 2, -1), (FACE, 0, 3, -1),
     (FACE, 0, 3, 0), (ALONG, 4, 2, 0), (CROSS, 5, 0, 0), (CROSS, 4, 0, 2), (BEGIN, 6, 0, 2), (ALONG, 3, 0, -1),
     (ALONG, 3, 0, 0), (ALONG, 3, 0, 1), (ALONG, 2, 3, -1), (ALONG, 2, 3, 0), (ALONG, 2, 3, 1),
     (FACE, 1, 3, -1), (FACE, 1, 3, 0), (ALONG, 4, 2, 1), (BEGIN, 5, 0, 1),),
    ((ALONG, 5, 2, -1), (FACE, 3, 2, -1), (FACE, 3, 2, 0), (CROSS, 6, 0, 0), (ALONG, 5, 2, 0), (DOWN, 0, 0, 0),
     (BEGIN, 6, 0, 1), (ALONG, 4, 0, -1), (ALONG, 4, 0, 0), (ALONG, 4, 0, 1),),
    ((ALONG, 3, 3, -1), (ALONG, 3, 3, 0), (ALONG, 3, 3, 1), (FACE, 2, 3, -1), (FACE, 2, 3, 0), (ACROSS, 4, 0, -1),
     (ACROSS, 4, 0, 0), (BEGIN, 7, 0, 2), (UP, 0, 0, 0), (CROSS, 5, 0, 1), (ALONG, 6, 2, -1), (CROSS, 6, 0, 1),
     (CROSS, 7, 0, 0),),
    ((DOWN, 0, 0, 1), (FACE, 4, 2, -1), (FACE, 4, 2, 0), (ALONG, 5, 0, -1), (ALONG, 5, 0, 0), (ALONG, 5, 0, 1),
     (ALONG, 4, 3, -1), (ALONG, 4, 3, 0), (ALONG, 4, 3, 1), (RELAY, 1, 0, 0), (DOWN, 1, 0, 0), (ALONG, 5, 2, 1),
     (UP, 0, 0, 1), (FACE, 3, 3, -1), (FACE, 3, 3, 0), (UP, 1, 0, 0), (UP, 1, 0, 1), (ALONG, 6, 2, 0),
     (ALONG, 7, 2, -1), (DOWN, 1, 0, 1),),
    ((UP, 2, 0, 0), (ALONG, 6, 0, -1), (ALONG, 6, 0, 0), (ALONG, 6, 0, 1), (DOWN, 2, 0, 0), (ALONG, 5, 3, -1),
     (ALONG, 5, 3, 0), (CROSS, 7, 0, 1), (ACROSS, 5, 0, -1), (ACROSS, 5, 0, 0), (FACE, 4, 3, -1),
     (FACE, 4, 3, 0), (ALONG, 5, 3, 1), (BEGIN, 7, 0, 1),),
    ((UP, 2, 0, 1), (ALONG, 6, 2, 1), (CROSS, 6, 0, 2), (DOWN, 2, 0, 1), (DOWN, 4, 0, 0), (FACE, 5, 2, -1),
     (FACE, 5, 2, 0), (DOWN, 3, 0, 1), (UP, 3, 0, 1), (UP, 3, 0, 0), (ALONG, 6, 3, -1), (ALONG, 6, 3, 0),
     (ALONG, 7, 0, -1), (ALONG, 7, 0, 0), (ALONG, 7, 0, 1), (FACE, 5, 3, -1), (FACE, 5, 3, 0), (ALONG, 7, 2, 0),
     (UP, 4, 0, 0), (ALONG, 6, 3, 1), (DOWN, 3, 0, 0), (ACROSS, 6, 0, -1), (ACROSS, 6, 0, 0), (ALONG, 7, 2, 1),
     (CROSS, 7, 0, 2), (UP, 4, 0, 1), (DOWN, 4, 0, 1), (FACE, 6, 2, -1), (FACE, 6, 2, 0), (FACE, 6, 3, -1),
     (FACE, 6, 3, 0), (ALONG, 7, 3, -1), (ALONG, 7, 3, 0), (ACROSS, 7, 0, -1), (ACROSS, 7, 0, 0),
     (FACE, 7, 2, -1), (FACE, 7, 2, 0), (ALONG, 7, 3, 1),),
    ((DOWN, 5, 0, 0), (DOWN, 5, 0, 1), (UP, 5, 0, 0), (UP, 5, 0, 1),),
    ((UP, 6, 0, 0), (RELAY, 5, 0, 0), (UP, 6, 0, 1), (DOWN, 6, 0, 1), (FACE, 7, 3, -1), (FACE, 7, 3, 0),
     (DOWN, 6, 0, 0),),
    ((DOWN, 7, 0, 0), (UP, 7, 0, 0), (DOWN, 7, 0, 1), (UP, 7, 0, 1),),
)


class Work:
    def __init__(self, n, refs, me):
        (self.gain, self.lengths, self.pages, self.freq, self.wide_gain, self.xbuf, self.raw, self.found,
         self.page_of, self.found_sem, self.cosine, self.sine) = refs
        self.n, self.me = n, me
        self.tok_rows, self.features = self.xbuf.shape
        self.length_each = self.tok_rows * n // 2
        self.first = lax.rem(me * self.tok_rows, self.length_each)

    def spread_gain(self):
        each = self.gain[...].astype(jnp.float32)
        rows = [each[i : i + 1, :] for i in range(self.features // HEAD)]
        self.wide_gain[...] = jnp.concatenate(rows, axis=1)

    def normalise(self, at, rows_here):
        xbuf = self.xbuf

        def body(i, carry):
            rows = pl.ds(pl.multiple_of(at + i * 32, 32), 32)
            wide = xbuf[rows, :].astype(jnp.float32)
            scale = lax.rsqrt(jnp.mean(wide * wide, axis=1, keepdims=True) + EPS)
            xbuf[rows, :] = (wide * scale * self.wide_gain[...]).astype(jnp.bfloat16)
            return carry

        lax.fori_loop(0, rows_here // 32, body, 0)

    def find_pages(self):
        page_count = self.tok_rows // PAGE
        lane = lax.broadcasted_iota(jnp.int32, self.found.shape, 1)
        page_of = jnp.full(self.found.shape, page_count, jnp.int32)
        for page in range(page_count):
            page_of = jnp.where(lane == lax.rem(self.pages[page], SLOTS), page, page_of)
        self.found[...] = page_of
        self.raw[page_count] = jnp.zeros(self.raw.shape[1:], jnp.bfloat16)
        copy = pltpu.make_async_copy(self.found, self.page_of, self.found_sem)
        copy.start()
        copy.wait()

    def angles(self, at, rows_here):
        def turn(i, carry):
            row_at = pl.multiple_of(at + i * 64, 64)
            row = lax.broadcasted_iota(jnp.int32, (64, HEAD), 0) + (self.first + row_at)
            lane = lax.broadcasted_iota(jnp.int32, (64, HEAD), 1)
            angle = row.astype(jnp.float32) * self.freq[...]
            self.cosine[pl.ds(row_at, 64), :] = jnp.cos(angle)
            sined = jnp.sin(angle)
            self.sine[pl.ds(row_at, 64), :] = jnp.where(lane < HEAD // 2, -sined, sined)
            return carry

        lax.fori_loop(0, rows_here // 64, turn, 0)

    def project(self, blocks, is_key, put):
        part = self.tok_rows // 2
        raw = None
        for ready, at, load in blocks:
            ready()
            weights = load()
            features = pl.ds(at, weights.shape[0])
            halves = [
                jnp.dot(
                    self.xbuf[i * part : (i + 1) * part, features],
                    weights,
                    preferred_element_type=jnp.float32,
                )
                for i in range(2)
            ]
            product = jnp.concatenate(halves, axis=0)
            raw = product if raw is None else raw + product
        if is_key:
            heads = []
            for head in range(weights.shape[1] // HEAD):
                one = raw[:, head * HEAD : (head + 1) * HEAD]
                heads.append(one * self.cosine[...] + pltpu.roll(one, HEAD // 2, 1) * self.sine[...])
            raw = jnp.concatenate(heads, axis=1)
        second_prompt = (self.me * self.tok_rows) // self.length_each
        limit = self.lengths[0] + second_prompt * (self.lengths[1] - self.lengths[0])
        row = lax.broadcasted_iota(jnp.int32, raw.shape, 0)
        raw = jnp.where(self.first + row < limit, raw, 0.0)
        wide = weights.shape[1]
        raw = raw.astype(jnp.bfloat16).reshape(self.tok_rows // PAGE, PAGE, wide)
        self.raw[0 : self.tok_rows // PAGE, :, 0:wide] = raw
        for slot in range(SLOTS):
            put(slot * PAGE, self.raw[self.page_of[0, slot]][:, 0:wide])


def copy_to(ref, send_sem, recv_sem, group_at, seq_at, dst=None):
    pltpu.make_async_remote_copy(
        src_ref=ref,
        dst_ref=ref if dst is None else dst,
        send_sem=send_sem,
        recv_sem=recv_sem,
        device_id={"group": group_at, "seq": seq_at},
        device_id_type=MESH,
    ).start()


def wait(ref, sem):
    pltpu.make_async_copy(ref, ref, sem).wait()


def line_kernel(
    n, tokens, gain, w_key, w_value, lengths, pages, freq, out,
    wide_gain, wbuf, xbuf, pbuf, rbuf, raw, found, page_of, found_sem, cosine, sine,
    load_sem, tok_sem, ys, yr, fr, fq, zi, zo, zr, xs, xo, xr, xq, cs, cr, cl, hs, hr, rs, rr,
):
    chunks, depth = wbuf.shape[0], wbuf.shape[1]
    half, width = wbuf.shape[5], wbuf.shape[6]
    per_kind = chunks // 2
    group = lax.axis_index("group")
    me = lax.axis_index("seq")
    core, y, z = lax.rem(me, 2), lax.rem(me // 2, 2), me // 4
    other_core, other_y, other_group = 1 - core, 1 - y, 1 - group
    high = z // (depth // 2)
    is_end = (z == 0) | (z == depth - 1)

    def at(p):
        return p + high * (depth - 1 - 2 * p)

    def seq_of(z_at, y_at, core_at):
        return (z_at * 2 + y_at) * 2 + core_at

    to_y = seq_of(z, other_y, core)
    to_core = seq_of(z, y, other_core)

    def piece(j, zz, yy, part):
        return wbuf.at[j, zz, yy, core, part]

    def line(j, zz, yy):
        return wbuf.at[j, zz, yy, core]

    def pair(j, zz, part):
        return wbuf.at[j, zz, :, core, part]

    def layer(j, zz):
        return wbuf.at[j, zz, :, core]

    def load(j):
        w_ref = w_key if j < per_kind else w_value
        columns = pl.ds((j % per_kind) * width, width)
        return [
            pltpu.make_async_copy(
                w_ref.at[pl.ds(part * half, half), columns], piece(j, z, y, part), load_sem.at[j, part]
            )
            for part in range(2)
        ]

    barrier = pltpu.get_barrier_semaphore()

    def greet(group_at, seq_at):
        pl.semaphore_signal(
            barrier, inc=1, device_id={"group": group_at, "seq": seq_at}, device_id_type=MESH
        )

    greet(other_group, me)
    for step in range(1, n):
        greet(group, lax.rem(me + step, n))
    for j in range(chunks):
        for copy in load(j):
            copy.start()
    token_copy = pltpu.make_async_copy(tokens, xbuf, tok_sem)
    token_copy.start()
    pl.semaphore_wait(barrier, n)

    def over_y(ref, j, sem):
        copy_to(ref, ys.at[j], sem, group, to_y)

    def over_x(ref, j, sem):
        copy_to(ref, xs.at[j], sem, other_group, me)

    def inward(ref, j, zz, p):
        copy_to(ref, zi.at[j], zr.at[j, zz], group, seq_of(at(p), y, core))

    def outward(ref, j, zz):
        copy_to(ref, zo.at[j], zr.at[j, zz], group, seq_of(at(0), y, core))

    def to_partner(j, zz, p=0):
        copy_to(layer(j, zz), cs.at[j], (cl if p == LAYERS - 1 else cr).at[j], group, to_core)

    def loaded(j):
        for copy in load(j):
            copy.wait()

    def end_waits(j, what, k):
        form, both = CHUNKS[j]
        zz = at(k)
        if what == CROSS:
            return [(line(j, z, other_y) if both else piece(j, z, other_y, group), yr.at[j])]
        if what == ACROSS:
            return [(piece(j, z, other_y, other_group), xo.at[j])]
        if what == ALONG:
            return [(pair(j, zz, group) if form == PAIRED else piece(j, zz, y, group), zr.at[j, zz])]
        from_x = (piece(j, zz, y, other_group), xr.at[j, zz])
        from_y = (piece(j, zz, other_y, group), fr.at[j, zz])
        if what == FACE:
            return [(pair(j, zz, other_group), xr.at[j, zz])] if form == PAIRED else [from_x]
        if what == SIDE:
            return [from_y]
        if form == SPLIT:
            return [from_y, (piece(j, zz, other_y, other_group), fq.at[j, zz])]
        return [from_x, (piece(j, zz, other_y, other_group), xq.at[j, zz])]

    def end_sends(j, what, k):
        form, both = CHUNKS[j]
        zz = at(k)
        partner = functools.partial(to_partner, j, zz, k)
        if what == BEGIN:
            mine = line(j, z, y) if both else piece(j, z, y, group)
            return [lambda: over_y(mine, j, yr.at[j]), lambda: inward(line(j, z, y), j, z, 1)]
        if what == CROSS:
            if both:
                return [lambda: inward(line(j, z, other_y), j, z, 1), lambda: to_partner(j, z)]
            return [
                lambda: inward(piece(j, z, other_y, group), j, z, 1),
                lambda: over_x(piece(j, z, other_y, group), j, xo.at[j]),
            ]
        if what == ACROSS:
            return [lambda: inward(piece(j, z, other_y, other_group), j, z, 1), lambda: to_partner(j, z)]
        if what == ALONG:
            one = piece(j, zz, y, group)
            by_x = lambda: over_x(one, j, xr.at[j, zz])
            by_y = lambda: over_y(one, j, fr.at[j, zz])
            if form == PAIRED:
                return [lambda: over_x(pair(j, zz, group), j, xr.at[j, zz])]
            return [by_x, by_y] if form == SPLIT else [by_y, by_x]
        if what == FACE and form == SPLIT:
            return [lambda: over_y(piece(j, zz, y, other_group), j, fq.at[j, zz])]
        if what == SIDE:
            return [lambda: over_x(piece(j, zz, other_y, group), j, xq.at[j, zz])]
        return [partner]

    def inner_waits(j, what, p):
        zz = at(p)
        if what == CROSS:
            return [(piece(j, z, other_y, group), yr.at[j])]
        if what == ACROSS:
            return [(piece(j, z, other_y, other_group), xo.at[j])]
        if what == ALONG:
            return [(layer(j, zz) if p == 0 else pair(j, zz, group), zr.at[j, zz])]
        return [(pair(j, zz, other_group), xr.at[j, zz])]

    def inner_sends(j, what, p):
        form, _ = CHUNKS[j]
        zz = at(p)
        if what == BEGIN:
            mine = piece(j, z, y, group)
            return [
                lambda: over_y(mine, j, yr.at[j]),
                lambda: outward(mine, j, z),
                lambda: inward(mine, j, z, 2),
            ]
        if what == CROSS:
            crossed = piece(j, z, other_y, group)
            out_too = [lambda: outward(crossed, j, z)] if form == PAIRED else []
            return [lambda: inward(crossed, j, z, 2)] + out_too + [lambda: over_x(crossed, j, xo.at[j])]
        if what == ACROSS:
            return [lambda: to_partner(j, z)]
        if what == ALONG and p == 0:
            return [lambda: inward(pair(j, zz, group), j, zz, 2), lambda: to_partner(j, zz)]
        if what == ALONG:
            kept = pair(j, zz, group) if form == PAIRED else piece(j, zz, y, group)
            return [lambda: outward(kept, j, zz), lambda: over_x(pair(j, zz, group), j, xr.at[j, zz])]
        return [lambda: to_partner(j, zz, p)]

    first_chunk = [sum(GROUPS[:g]) for g in range(len(GROUPS))]

    def spot(g, region):
        j, wide = first_chunk[g], GROUPS[g] * width
        rows = pl.ds(region * BLOCK, BLOCK)
        return (
            pbuf.at[g, rows, pl.ds(0, wide)],
            out.at[j // per_kind, rows, pl.ds((j % per_kind) * width, wide)],
        )

    def page_to(g, region):
        src, dst = spot(g, region)
        there = lax.rem(me + region - REACH + n, n)
        z_there, y_there = there // 4, lax.rem(there // 2, 2)

        def direct():
            copy_to(src, hs.at[g, region], hr.at[g, region], group, there, dst)

        if g not in RELAYED:
            direct()
            return
        slot = 0 if abs(region - REACH) == 2 else 1
        around = ((z_there == 0) | (z_there == depth - 1)) & (z_there != z)
        z_by = 1 + (z_there // (depth - 1)) * (depth - 3)
        by = seq_of(z_by, y_there, lax.rem(there, 2))

        @pl.when(around)
        def _():
            held = rbuf.at[RELAYED.index(g), slot, :, pl.ds(0, GROUPS[g] * width)]
            copy_to(src, hs.at[g, region], rr.at[g, slot], group, by, held)

        @pl.when(jnp.logical_not(around))
        def _():
            direct()

    def pages_on_chip(g):
        src, dst = spot(g, REACH)
        pltpu.make_async_copy(src, dst, hr.at[g, REACH]).start()
        for region, on in ((3, core == 0), (1, core == 1)):
            @pl.when(on)
            def _():
                src, dst = spot(g, region)
                copy_to(src, hs.at[g, region], hr.at[g, region], group, to_core, dst)

    def pages_off_chip(g, way, which):
        if which == 0:
            page_to(g, 4 if way == UP else 0)
            return

        @pl.when(core == (1 if way == UP else 0))
        def _():
            page_to(g, 3 if way == UP else 1)

    def pass_pages(g):
        def one(slot, region):
            held = rbuf.at[RELAYED.index(g), slot, :, pl.ds(0, GROUPS[g] * width)]
            wait(held, rr.at[g, slot])
            _, dst = spot(g, region)
            copy_to(held, rs.at[g, slot], hr.at[g, region], group, seq_of(at(0), y, core), dst)

        for side, regions in ((0, (4, 3)), (1, (0, 1))):
            @pl.when(y == side)
            def _():
                one(0, regions[0])

                @pl.when(core == side)
                def _():
                    one(1, regions[1])

    def run(steps, waits, sends, seen):
        for what, j, k, which in steps:
            if what in (UP, DOWN):
                pages_off_chip(j, what, which)
            elif what == RELAY:
                pass_pages(j)
            elif what == BEGIN:
                if j not in seen:
                    seen.add(j)
                    loaded(j)
                sends(j, what, k)[which]()
            elif which < 0:
                for ref, sem in waits(j, what, k):
                    wait(ref, sem)
            else:
                sends(j, what, k)[which]()

    work = Work(n, (gain, lengths, pages, freq, wide_gain, xbuf, raw, found, page_of, found_sem, cosine, sine), me)
    tok_rows = work.tok_rows

    def project(g):
        at_chunk, wide = first_chunk[g], GROUPS[g] * width
        here = range(at_chunk, at_chunk + GROUPS[g])
        each = work.features // depth

        def block(layers, count_of, sems):
            def ready():
                for j in here:
                    wait(wbuf.at[j, layers, :, other_core], sems.at[j])

            def read():
                parts = [wbuf[j, layers].reshape(count_of * each, width) for j in here]
                return parts[0] if len(parts) == 1 else jnp.concatenate(parts, axis=1)

            return ready, read

        far = (1 - high) * (depth - 1)
        ready, read = block(pl.ds(high, depth - 1), depth - 1, cr)
        ready_far, read_far = block(pl.ds(far, 1), 1, cl)
        blocks = [
            (ready, pl.multiple_of(high * each, each), read),
            (ready_far, pl.multiple_of(far * each, each), read_far),
        ]

        def put(at_row, page):
            pbuf[g, at_row : at_row + PAGE, 0:wide] = page

        work.project(blocks, at_chunk < per_kind, put)
        pages_on_chip(g)

    sixteenth = tok_rows // 16
    jobs = [lambda: (work.spread_gain(), token_copy.wait())]
    jobs += [functools.partial(work.normalise, i * sixteenth, sixteenth) for i in range(16)]
    jobs += [work.find_pages]
    jobs += [functools.partial(work.angles, i * (tok_rows // 2), tok_rows // 2) for i in range(2)]
    jobs, projects = iter(jobs), iter(range(len(GROUPS)))
    inner, second = jnp.logical_not(is_end), y != high
    first = jnp.logical_not(second)
    kinds = (
        (is_end & first, END_FIRST, end_waits, end_sends, set()),
        (is_end & second, END_SECOND, end_waits, end_sends, set()),
        (inner & first, INNER_FIRST, inner_waits, inner_sends, set()),
        (inner & second, INNER_SECOND, inner_waits, inner_sends, set()),
    )
    for stretch in range(len(COMPUTE) + 1):
        if stretch:
            if COMPUTE[stretch - 1]:
                project(next(projects))
            else:
                next(jobs)()
        for here, steps, waits, sends, seen in kinds:
            if steps[stretch]:

                @pl.when(here)
                def _():
                    run(steps[stretch], waits, sends, seen)

    def count(pieces, sem):
        wait(xbuf.at[pl.ds(0, half), pl.ds(0, pieces * width)], sem)

    for j in range(chunks):
        form, both = CHUNKS[j]
        wait(wbuf.at[j, :, :, core], cs.at[j])

        @pl.when(is_end)
        def _():
            far = depth - 1
            count((2 if both else 1) + far * {PAIRED: 0, SPLIT: 2, TURNED: 1}[form], ys.at[j])
            count(far * {PAIRED: 2, SPLIT: 1, TURNED: 2}[form] + (0 if both else 1), xs.at[j])
            count(4, zi.at[j])

        @pl.when(jnp.logical_not(is_end))
        def _():
            count(1, ys.at[j])
            count(2 * depth - 3, xs.at[j])
            count(4, zi.at[j])
            count((depth - 1) * (2 if form == PAIRED else 1), zo.at[j])

    for g in range(len(GROUPS)):
        for region in range(REGIONS):
            src, dst = spot(g, region)
            wait(dst, hr.at[g, region])
            if region != REACH:
                wait(src, hs.at[g, region])
        if g in RELAYED:
            held = rbuf.at[RELAYED.index(g), 0, :, pl.ds(0, GROUPS[g] * width)]

            @pl.when(jnp.logical_not(is_end))
            def _():
                wait(held, rs.at[g, 0])

                @pl.when(core == y)
                def _():
                    wait(held, rs.at[g, 1])


def loop_kernel(
    n, tokens, gain, w_key, w_value, lengths, pages, freq, out,
    wide_gain, wbuf, xbuf, pbuf, raw, found, page_of, found_sem, cosine, sine,
    load_sem, tok_sem, ys, yr, zs, zr, xs, xr, cs, cr, hs, hr,
):
    chunks, depth = wbuf.shape[0], wbuf.shape[1]
    half, width = wbuf.shape[5], wbuf.shape[6]
    per_kind = chunks // 2
    group = lax.axis_index("group")
    me = lax.axis_index("seq")
    core, y, z = lax.rem(me, 2), lax.rem(me // 2, 2), me // 4
    other_core, other_y, other_group = 1 - core, 1 - y, 1 - group

    def seq_of(z_at, y_at, core_at):
        return (z_at * 2 + y_at) * 2 + core_at

    def piece(j, z_at, y_at, part):
        return wbuf.at[j, z_at, y_at, core, part]

    loads = []
    for j in range(chunks):
        w_ref = w_key if j < per_kind else w_value
        columns = pl.ds((j % per_kind) * width, width)
        for part in range(2):
            copy = pltpu.make_async_copy(
                w_ref.at[pl.ds(part * half, half), columns], piece(j, z, y, part), load_sem.at[j, part]
            )
            copy.start()
            loads.append(copy)
    token_copy = pltpu.make_async_copy(tokens, xbuf, tok_sem)
    token_copy.start()

    to_y = seq_of(z, other_y, core)
    to_core = seq_of(z, y, other_core)
    has_up, has_down = z + 1 < depth, z > 0
    up = seq_of(lax.rem(z + 1, depth), y, core)
    down = seq_of(lax.rem(z + depth - 1, depth), y, core)

    barrier = pltpu.get_barrier_semaphore()

    def greet(group_at, seq_at):
        pl.semaphore_signal(
            barrier, inc=1, device_id={"group": group_at, "seq": seq_at}, device_id_type=MESH
        )

    for seq_at in (up, down, to_y, to_core):
        greet(group, seq_at)
    greet(other_group, me)
    for region in range(REGIONS):
        if region != REACH:
            greet(group, lax.rem(me + region - REACH + n, n))
    pl.semaphore_wait(barrier, 5 + REGIONS - 1)

    def to_partner(j, ref):
        copy_to(ref, cs.at[j], cr.at[j], group, to_core)

    def go(j, z_at, y_at, k, way):
        @pl.when(has_up if way == 0 else has_down)
        def _():
            copy_to(piece(j, z_at, y_at, group), zs.at[j, way, k], zr.at[j, y_at, z_at], group,
                    up if way == 0 else down)

    def begin(j):
        for part in (0, 1):
            loads[2 * j + part].wait()
        for part in (0, 1):
            copy_to(piece(j, z, y, part), ys.at[j], yr.at[j, part], group, to_y)
            to_partner(j, piece(j, z, y, part))
        go(j, z, y, 0, 0)
        go(j, z, y, 0, 1)

    def cross(j):
        for part in (0, 1):
            wait(piece(j, z, other_y, part), yr.at[j, part])
            to_partner(j, piece(j, z, other_y, part))
        go(j, z, other_y, 0, 0)
        go(j, z, other_y, 0, 1)

    def both(k, visit):
        @pl.when(z - k >= 0)
        def _():
            visit(z - k, 0)

        @pl.when(z + k < depth)
        def _():
            visit(z + k, 1)

    def along(j, k):
        def visit(zz, way):
            for y_at in (y, other_y):
                ref = piece(j, zz, y_at, group)
                wait(ref, zr.at[j, y_at, zz])
                go(j, zz, y_at, k, way)
                copy_to(ref, xs.at[j], xr.at[j, y_at, zz], other_group, me)
                to_partner(j, ref)

        both(k, visit)

    def finish(j, k):
        def visit(zz, way):
            for y_at in (y, other_y):
                ref = piece(j, zz, y_at, other_group)
                wait(ref, xr.at[j, y_at, zz])
                to_partner(j, ref)

        both(k, visit)

    work = Work(n, (gain, lengths, pages, freq, wide_gain, xbuf, raw, found, page_of, found_sem, cosine, sine), me)

    def project(j):
        wait(wbuf.at[j, :, :, other_core], cr.at[j])
        for at in range(0, width, TILE):
            def put(at_row, page):
                pbuf[j, at_row : at_row + PAGE, at : at + TILE] = page

            weights = wbuf[j, :, :, :, :, :, at : at + TILE].reshape(work.features, TILE)
            work.project([(lambda: None, 0, lambda: weights)], j < per_kind, put)

    def spot(j, region):
        rows = pl.ds(region * BLOCK, BLOCK)
        return (
            pbuf.at[j, rows, :],
            out.at[j // per_kind, rows, pl.ds((j % per_kind) * width, width)],
        )

    def hand_over(j):
        for region in range(REGIONS):
            src, dst = spot(j, region)
            if region == REACH:
                pltpu.make_async_copy(src, dst, hr.at[j, region]).start()
            else:
                copy_to(src, hs.at[j, region], hr.at[j, region], group,
                        lax.rem(me + region - REACH + n, n), dst)

    for j in range(chunks):
        begin(j)
    work.spread_gain()
    token_copy.wait()
    work.normalise(0, work.tok_rows)
    work.find_pages()
    work.angles(0, work.tok_rows)
    for j in range(chunks):
        cross(j)
        lax.fori_loop(1, depth, lambda k, carry: (along(j, k), carry)[1], 0)
        lax.fori_loop(1, depth, lambda k, carry: (finish(j, k), carry)[1], 0)
        project(j)
        hand_over(j)

    for j in range(chunks):
        wait(wbuf.at[j, z, y, core], ys.at[j])
        wait(wbuf.at[j, 1:, :, core, group], xs.at[j])
        wait(wbuf.at[j, :, :, core], cs.at[j])
        sent = wbuf.at[j, 0, :, core, group]

        def drain(k, carry):
            @pl.when(has_up & (z - k >= 0))
            def _():
                wait(sent, zs.at[j, 0, k])

            @pl.when(has_down & (z + k < depth))
            def _():
                wait(sent, zs.at[j, 1, k])

            return carry

        lax.fori_loop(0, depth, drain, 0)
        for region in range(REGIONS):
            src, dst = spot(j, region)
            wait(dst, hr.at[j, region])
            if region != REACH:
                wait(src, hs.at[j, region])


def on_device(n, tokens, norm_gain, w_key, w_value, lengths, page_table):
    tok_rows, features = tokens.shape
    columns = w_key.shape[1]
    freq = ROPE_THETA ** (-(np.arange(HEAD // 2) * 2.0 / HEAD))
    freq = np.concatenate([freq, freq]).astype(np.float32)[None, :]
    depth = n // 4
    half = w_key.shape[0] // 2
    dma = pltpu.SemaphoreType.DMA
    vmem = pl.BlockSpec(memory_space=pltpu.VMEM)
    smem = pl.BlockSpec(memory_space=pltpu.SMEM)
    hbm = pl.BlockSpec(memory_space=pl.ANY)
    in_line = depth == LAYERS
    chunks = len(CHUNKS) if in_line else LOOP_CHUNKS
    groups = len(GROUPS) if in_line else chunks
    width = 2 * columns // chunks
    wide = width * max(GROUPS) if in_line else width
    scratch = [
        pltpu.VMEM((1, features), jnp.float32),
        pltpu.VMEM((chunks, depth, 2, 2, 2, half, width), jnp.bfloat16),
        pltpu.VMEM((tok_rows, features), jnp.bfloat16),
        pltpu.VMEM((groups, ROWS, wide), jnp.bfloat16),
    ]
    if in_line:
        scratch.append(pltpu.VMEM((max(len(RELAYED), 1), 2, BLOCK, wide), jnp.bfloat16))
    scratch += [
        pltpu.VMEM((tok_rows // PAGE + 1, PAGE, TILE), jnp.bfloat16),
        pltpu.VMEM((1, HEAD), jnp.int32),
        pltpu.SMEM((1, HEAD), jnp.int32),
        dma,
        pltpu.VMEM((tok_rows, HEAD), jnp.float32),
        pltpu.VMEM((tok_rows, HEAD), jnp.float32),
        dma((chunks, 2)),
        dma,
    ]
    each, by_layer, by_region = dma((chunks,)), dma((chunks, depth)), dma((groups, REGIONS))
    if in_line:
        slots = dma((groups, 2))
        scratch += [each, each, by_layer, by_layer, each, each, by_layer, each, each, by_layer, by_layer,
                    each, each, each, by_region, by_region, slots, slots]
    else:
        by_line = dma((chunks, 2, depth))
        scratch += [each, dma((chunks, 2)), by_line, by_line, each, by_line, each, each,
                    by_region, by_region]
    cache = pl.pallas_call(
        functools.partial(line_kernel if in_line else loop_kernel, n),
        out_shape=pltpu.VMEM((2, ROWS, columns), jnp.bfloat16),
        in_specs=[hbm, vmem, hbm, hbm, smem, smem, vmem],
        out_specs=vmem,
        scratch_shapes=scratch,
        compiler_params=pltpu.CompilerParams(
            collective_id=0, has_side_effects=True, vmem_limit_bytes=60 * 2**20
        ),
    )(tokens, norm_gain.reshape(-1, HEAD), w_key, w_value, lengths, page_table, freq)
    return cache.reshape(2, SLOTS, PAGE, columns)


def solution(mesh):
    placed = (
        P(("group", "seq"), None),
        P(),
        P("seq", None),
        P("seq", None),
        P("group"),
        P(("group", "seq")),
    )
    return jax.shard_map(
        functools.partial(on_device, mesh.shape["seq"]),
        mesh=mesh,
        in_specs=placed,
        out_specs=P(None, ("group", "seq"), None, None),
        check_vma=False,
    )
```
